256 devices in a mesh: blk: 16 (over x_lo, z), tgt: 16 (over y, x_hi, core).
Axes of the slice: x: 4 (x_hi: 2, x_lo: 2; x = x_hi * 2 + x_lo), y: 4, z: 8, core: 2. Of those that a mesh axis runs over, the one named last changes fastest.
Arguments:
- sources: float32 [16384, 128], P('blk'), may hold values from -0.5 to 0.5, as said below
- targets: float32 [65536, 128], P(('blk', 'tgt')), may hold values from -0.5 to 0.5, as said below
- duals_init: float32 [65536], P(('blk', 'tgt')), may hold values from -1.5 to 1.5
Outputs:
- source_duals: float32 [16384], P('blk')
- target_duals: float32 [65536], P(('blk', 'tgt'))
The draws below stay inside these ranges and needn't reach their ends.
Inputs may be any that keep to these rules, and one draw needn't show every extreme that they name: `sources`: coordinates of the source points. `targets`: coordinates of the target points.
All inputs are finite; a program needn't handle non-finite values.
Results may differ from the reference program's by a relative error of at most 0.0001.
Values sent between devices are 32-bit elements; how exact they have to be, the bound alone decides.
No kernel may reach another device: no remote copies, remote signals or barrier semaphores. Data moves between devices by JAX's collectives and lax.ppermute only.
A program may use at most 64 MiB of HBM per device.

```python
import jax
import jax.numpy as jnp
from jax import lax

D = 128
ROWS_DEV = 1024
TGT_DEV = 256
ITERS = 2
N_SRC = 16384
N_DST = 65536


def common_offset(key):
    inner = jax.random.fold_in(key, 11)
    size_key, sign_key = jax.random.split(inner)
    magnitude = jax.random.uniform(size_key, (D,), jnp.float32, 0.15, 0.25)
    signs = jnp.where(jax.random.bernoulli(sign_key, 0.5, (D,)), 1.0, -1.0)
    return magnitude * signs


def cloud_points(key, salt, count):
    offset = common_offset(key)
    inner = jax.random.fold_in(key, salt)
    base_key, pick_key, sign_key, size_key = jax.random.split(inner, 4)
    base = 0.0625 * jax.random.truncated_normal(base_key, -6.0, 6.0, (count, D), jnp.float32)
    chosen = jax.random.randint(pick_key, (count,), 0, 48) == 0
    signs = jnp.where(jax.random.bernoulli(sign_key, 0.5, (count, D)), 1.0, -1.0)
    strength = jax.random.uniform(size_key, (count, 1), jnp.float32, 0.6, 1.0)
    far_part = 0.45 * strength * signs
    local = jnp.where(chosen[:, None], far_part, base)
    return jnp.clip(offset[None, :] + local, -0.5, 0.5)


def draw_sources(key, part):
    return cloud_points(key, 3, N_SRC)


def draw_targets(key, part):
    return cloud_points(key, 5, N_DST)


def steps_of(stream_key, shape, cuts, smallest, high):
    loudness, own = 1.0, jax.random.fold_in(stream_key, 6)
    for dim, shards_of in cuts:
        draws = jnp.exp(jax.random.uniform(jax.random.fold_in(own, dim), (shards_of,), jnp.float32, smallest / len(cuts), high / len(cuts)))
        loudness = loudness * jnp.repeat(draws, shape[dim] // shards_of).reshape([-1 if axis == dim else 1 for axis in range(len(shape))])
    return loudness


def scatter_about(own_key, extent, deviation, bound, pieces=(), held_as=jnp.bfloat16):
    entries = deviation * jax.random.normal(own_key, extent, jnp.float32)
    if pieces:
        entries = entries * steps_of(own_key, extent, pieces, -0.22, 0.18)
    return jnp.clip(entries, -bound, bound).astype(held_as)


def setup_inputs(seed: int = 0) -> dict:
    arg_keys = jax.random.split(jax.random.key(seed), 4)
    sources = draw_sources(jax.random.fold_in(arg_keys[3], 71), 0)
    targets = draw_targets(jax.random.fold_in(arg_keys[3], 71), 0)
    duals_init = scatter_about(arg_keys[2], (N_DST,), 0.3, 1.5, ((0, 256),), jnp.float32)
    return {"sources": sources, "targets": targets, "duals_init": duals_init}


EPS = 0.05


def block_lse(left_blk, left_norm, right, right_norm, right_pots):
    cross = jnp.dot(left_blk, right.T, preferred_element_type=jnp.float32, precision=lax.Precision.HIGHEST)
    cost_tile = left_norm[:, None] + right_norm[None, :] - 2.0 * cross
    scores = (right_pots[None, :] - cost_tile) / EPS
    maxima = jnp.max(scores, axis=1)
    return maxima + jnp.log(jnp.sum(jnp.exp(scores - maxima[:, None]), axis=1))


def half_step(left, left_norm, right, right_norm, right_pots, block):
    count = left.shape[0] // block
    left_blocks = left.reshape(count, block, left.shape[1])
    norm_blocks = left_norm.reshape(count, block)
    result = lax.map(lambda pair: block_lse(pair[0], pair[1], right, right_norm, right_pots), (left_blocks, norm_blocks))
    return EPS * (-jnp.log(jnp.float32(right.shape[0]))) - EPS * result.reshape(-1)


def reference(sources, targets, duals_init):
    src_norm = jnp.sum(sources * sources, axis=1)
    dst_norm = jnp.sum(targets * targets, axis=1)
    target_pots = duals_init
    source_pots = jnp.zeros_like(src_norm)
    for repeat in range(ITERS):
        source_pots = half_step(sources, src_norm, targets, dst_norm, target_pots, ROWS_DEV)
        target_pots = half_step(targets, dst_norm, sources, src_norm, source_pots, TGT_DEV)
    return source_pots, target_pots
```

```python
import functools
import math

import jax
import jax.numpy as jnp
from jax import lax
from jax.experimental import pallas as pl
from jax.experimental.pallas import tpu as pltpu
from jax.sharding import Mesh
from jax.sharding import PartitionSpec as P

EPS = 0.05
SCALE = math.log2(math.e) / EPS
LOG2E = math.log2(math.e)
N_SRC = 16384
N_DST = 65536
ROWS = 1024
COLS = 256
RING = 8
PLANE = 32
WIDE = 2 * ROWS
PACK = COLS + 8
OFFSETS = (0, -1, 1, -2, 2, -3, 3, -4)
GROUPS = (3, 2, 2, 1)
MIB = 1024 * 1024

BLK = ("xl", "z")
TGT = ("y", "xh", "core")
PLANE_AXES = ("xl", "y", "xh", "core")

VMEM = pl.BlockSpec(memory_space=pltpu.VMEM)
SMEM = pl.BlockSpec(memory_space=pltpu.SMEM)


def log2(x):
    return jnp.log(x) * LOG2E


def diagonal():
    shape = (128, 128)
    return lax.broadcasted_iota(jnp.int32, shape, 0) == lax.broadcasted_iota(jnp.int32, shape, 1)


def as_column(eye, row):
    return jnp.sum(jnp.where(eye, row, 0.0), axis=1, keepdims=True)


def as_row(eye, column):
    return jnp.sum(jnp.where(eye, column, 0.0), axis=0, keepdims=True)


def tree(op, parts):
    parts = list(parts)
    while len(parts) > 1:
        parts = [op(*parts[k : k + 2]) if k + 1 < len(parts) else parts[k] for k in range(0, len(parts), 2)]
    return parts[0]


def three_parts(x):
    high = x.astype(jnp.bfloat16)
    rest = x - high.astype(jnp.float32)
    mid = rest.astype(jnp.bfloat16)
    low = (rest - mid.astype(jnp.float32)).astype(jnp.bfloat16)
    return high, mid, low


def online(scores, state):
    high = jnp.max(scores, axis=0)
    if state is None:
        return high, jnp.sum(jnp.exp2(scores - high[None]), axis=0)
    high = jnp.maximum(high, state[0])
    total = state[1] * jnp.exp2(state[0] - high) + jnp.sum(jnp.exp2(scores - high[None]), axis=0)
    return high, total


def over_sublanes(high, total):
    top = jnp.max(high, axis=0, keepdims=True)
    return top + log2(jnp.sum(total * jnp.exp2(high - top), axis=0, keepdims=True))


def joined(parts):
    top = jnp.max(parts, axis=0)
    return top + log2(jnp.sum(jnp.exp2(parts - top[None]), axis=0))


def put_rows(where_ref, rows_ref, lse_tiles):
    mine = where_ref[1]
    halves = [jnp.concatenate(lse_tiles[8 * h : 8 * h + 8], axis=0) for h in range(2)]
    for h in range(2):
        half = mine if h == 0 else 1 - mine
        for peer in range(PLANE):
            rows_ref[peer, half] = halves[h]


def build_kernel(first, last, count, *refs):
    refs = list(refs)
    where_ref = refs.pop(0)
    if first:
        sources = refs.pop(0), refs.pop(0)
    else:
        x_ref, high_in, total_in = refs.pop(0), refs.pop(0), refs.pop(0)
    blocks = [refs.pop(0) for _ in range(count)]
    tile_ref = refs.pop(0)
    if first:
        x_ref, src_norm_ref, dst_norm_ref = refs.pop(0), refs.pop(0), refs.pop(0)
    if last:
        rows_ref = refs.pop(0)
    else:
        high_out, total_out = refs.pop(0), refs.pop(0)
    eye = diagonal()
    if first:
        for h in range(2):
            x = sources[h][...]
            high, mid, low = three_parts(x * (2.0 * SCALE))
            x_ref[h * ROWS : (h + 1) * ROWS, :] = jnp.concatenate([high, high, mid, mid, low, high], axis=1)
            if h == 0:
                norms = jnp.sum(x * x, axis=1, keepdims=True)
                for c in range(ROWS // 128):
                    src_norm_ref[c : c + 1, :] = as_row(eye, norms[c * 128 : (c + 1) * 128])
    parts, starts = [], []
    for b in range(count):
        y = blocks[b][0:COLS, :]
        norms = jnp.sum(y * y, axis=1, keepdims=True)
        if first and b == 0:
            for c in range(COLS // 128):
                dst_norm_ref[c : c + 1, :] = as_row(eye, norms[c * 128 : (c + 1) * 128])
        pots = [as_column(eye, blocks[b][COLS + c : COLS + c + 1, :]) for c in range(COLS // 128)]
        starts.append((jnp.concatenate(pots, axis=0) - norms) * SCALE)
        high, mid, low = three_parts(y)
        parts.append(jnp.concatenate([high, mid, high, mid, high, low], axis=1))
    step = 512
    lse_tiles = []
    for a in range(WIDE // step):
        lanes = slice(a * step, (a + 1) * step)
        state = None if first else (high_in[:, lanes], total_in[:, lanes])
        for b in range(count):
            piece = lax.dot_general(
                parts[b], x_ref[lanes, :], (((1,), (1,)), ((), ())), preferred_element_type=jnp.float32
            )
            tile_ref[b, :, lanes] = piece
            state = online((piece + starts[b]).reshape(COLS // 8, 8, step), state)
        if last:
            done = over_sublanes(*state)
            lse_tiles += [done[:, k * 128 : (k + 1) * 128] for k in range(step // 128)]
        else:
            high_out[:, lanes], total_out[:, lanes] = state
    if last:
        put_rows(where_ref, rows_ref, lse_tiles)


def build(where, count, blocks, sources=None, state=None, last=False):
    first = sources is not None
    args = [where, *(sources if first else state), *blocks]
    f32, bf16 = jnp.float32, jnp.bfloat16
    outs = [jax.ShapeDtypeStruct((count, COLS, WIDE), f32)]
    if first:
        outs += [
            jax.ShapeDtypeStruct((WIDE, 768), bf16),
            jax.ShapeDtypeStruct((ROWS // 128, 128), f32),
            jax.ShapeDtypeStruct((COLS // 128, 128), f32),
        ]
    if last:
        outs.append(jax.ShapeDtypeStruct((PLANE, 2, ROWS // 128, 128), f32))
    else:
        outs += [jax.ShapeDtypeStruct((8, WIDE), f32)] * 2
    return pl.pallas_call(
        functools.partial(build_kernel, first, last, count),
        out_shape=outs,
        in_specs=[SMEM] + [VMEM] * (len(args) - 1),
        out_specs=[VMEM] * len(outs),
        compiler_params=pltpu.CompilerParams(vmem_limit_bytes=28 * MIB),
        cost_estimate=pl.CostEstimate(
            flops=2 * count * COLS * WIDE * 768, bytes_accessed=4 * MIB, transcendentals=count * COLS * WIDE
        ),
        name=f"build_{count}_{int(first)}{int(last)}",
    )(*args)


def tile_blocks(tiles):
    return [(tiles[g], b) for g, count in enumerate(GROUPS) for b in range(count)]


def columns_kernel(copies, where_ref, rows_ref, src_norm_ref, *refs):
    tiles, refs = refs[: len(GROUPS)], refs[len(GROUPS) :]
    if copies:
        cols_ref, high_scr, total_scr = refs
    else:
        cols_ref, source_pots_ref, high_scr, total_scr = refs
    z, mine = where_ref[0], where_ref[1]
    eye = diagonal()
    pots = []
    for h in range(2):
        half = mine if h == 0 else 1 - mine
        lse = joined(rows_ref[:, half])
        u = -math.log2(N_DST) - lse
        if h == 0 and not copies:
            source_pots_ref[...] = u * (1.0 / SCALE) + src_norm_ref[...]
        pots += [jnp.broadcast_to(u[c : c + 1, :], (8, 128)) for c in range(ROWS // 128)]
    unroll = 4
    for k, (tile_ref, b) in enumerate(tile_blocks(tiles)):

        def rows_of(i, carry, tile_ref=tile_ref, b=b, k=k):
            for g in range(unroll):
                at = pl.ds(pl.multiple_of((i * unroll + g) * 8, 8), 8)
                scores = [tile_ref[b, at, c * 128 : (c + 1) * 128] + pots[c] for c in range(16)]
                high = tree(jnp.maximum, scores)
                total = tree(jnp.add, [jnp.exp2(s - high) for s in scores])
                high_scr[k, at, :] = high
                total_scr[k, at, :] = total
            return carry

        lax.fori_loop(0, COLS // 8 // unroll, rows_of, 0)
    for k, offset in enumerate(OFFSETS):
        at = lax.rem(z + (offset + RING), RING)
        for c in range(COLS // 128):
            rows = slice(c * 128, (c + 1) * 128)
            high = high_scr[k, rows, :]
            top = jnp.max(high, axis=1, keepdims=True)
            total = jnp.sum(total_scr[k, rows, :] * jnp.exp2(high - top), axis=1, keepdims=True)
            lse = as_row(eye, top + log2(total))
            if copies:
                for peer in range(RING):
                    cols_ref[peer, at, c : c + 1, :] = lse
            else:
                cols_ref[at, c : c + 1, :] = lse


def columns(where, rows, src_norm, tiles, copies):
    f32 = jnp.float32
    block = (RING, COLS // 128, 128)
    if copies:
        outs = [jax.ShapeDtypeStruct((RING, *block), f32)]
    else:
        outs = [jax.ShapeDtypeStruct(block, f32), jax.ShapeDtypeStruct((ROWS // 128, 128), f32)]
    return pl.pallas_call(
        functools.partial(columns_kernel, copies),
        out_shape=outs,
        in_specs=[SMEM] + [VMEM] * (2 + len(tiles)),
        out_specs=[VMEM] * len(outs),
        scratch_shapes=[pltpu.VMEM((RING, COLS, 128), f32)] * 2,
        compiler_params=pltpu.CompilerParams(vmem_limit_bytes=28 * MIB),
        cost_estimate=pl.CostEstimate(flops=5 * WIDE * WIDE, bytes_accessed=4 * MIB, transcendentals=WIDE * WIDE),
        name="columns_all" if copies else "columns_own",
    )(where, rows, src_norm, *tiles)


def rows_kernel(where_ref, cols_ref, *refs):
    tiles, (rows_ref, pots_scr, lse_scr) = refs[: len(GROUPS)], refs[len(GROUPS) :]
    z = where_ref[0]
    eye = diagonal()
    for k, offset in enumerate(OFFSETS):
        at = lax.rem(z + (offset + RING), RING)
        w = -math.log2(N_SRC) - joined(cols_ref[:, at])
        for c in range(COLS // 128):
            column = as_column(eye, w[c : c + 1, :])
            pots_scr[2 * k + c] = jnp.broadcast_to(column, (128, 128)).reshape(16, 8, 128)

    def lanes_of(i, carry):
        states = [None, None]
        for k, (tile_ref, b) in enumerate(tile_blocks(tiles)):
            for c in range(COLS // 128):
                pots = pots_scr[2 * k + c]
                for t in range(2):
                    lanes = pl.ds(pl.multiple_of(i * 256 + t * 128, 128), 128)
                    scores = tile_ref[b, c * 128 : (c + 1) * 128, lanes].reshape(16, 8, 128) + pots
                    states[t] = online(scores, states[t])
        lse_scr[i] = jnp.concatenate([over_sublanes(*states[t]) for t in range(2)], axis=0)
        return carry

    lax.fori_loop(0, WIDE // 256, lanes_of, 0)
    put_rows(where_ref, rows_ref, [lse_scr[i, t : t + 1, :] for i in range(WIDE // 256) for t in range(2)])


def rows(where, cols, tiles):
    f32 = jnp.float32
    return pl.pallas_call(
        rows_kernel,
        out_shape=jax.ShapeDtypeStruct((PLANE, 2, ROWS // 128, 128), f32),
        in_specs=[SMEM] + [VMEM] * (1 + len(tiles)),
        out_specs=VMEM,
        scratch_shapes=[pltpu.VMEM((16, 16, 8, 128), f32), pltpu.VMEM((WIDE // 256, 2, 128), f32)],
        compiler_params=pltpu.CompilerParams(vmem_limit_bytes=28 * MIB),
        cost_estimate=pl.CostEstimate(flops=5 * WIDE * WIDE, bytes_accessed=4 * MIB, transcendentals=WIDE * WIDE),
        name="rows_all",
    )(where, cols, *tiles)


def finish_kernel(cols_ref, dst_norm_ref, out_ref):
    w = -math.log2(N_SRC) - joined(cols_ref[...])
    out_ref[...] = w * (1.0 / SCALE) + dst_norm_ref[...]


def shifted(x, axis, by):
    count = lax.axis_size(axis)
    return lax.ppermute(x, axis, [(i, (i + by) % count) for i in range(count)])


def body(sources, targets, duals_init):
    where = jnp.stack([lax.axis_index("z"), lax.axis_index("xl")]).astype(jnp.int32)
    packed = jnp.concatenate([targets, jnp.pad(duals_init.reshape(2, 128), ((0, 6), (0, 0)))], axis=0)
    others = shifted(sources, "xl", 1)
    up, down, ring = [packed], [packed], [packed]
    for step in range(1, RING // 2 + 1):
        up.append(shifted(up[-1], "z", 1))
        ring.append(up[-1])
        if step < RING // 2:
            down.append(shifted(down[-1], "z", -1))
            ring.append(down[-1])
    tiles, at = [], 0
    for g, count in enumerate(GROUPS):
        blocks, at = ring[at : at + count], at + count
        last = g == len(GROUPS) - 1
        if g == 0:
            tile, x, src_norm, dst_norm, *state = build(where, count, blocks, sources=(sources, others))
        else:
            tile, *state = build(where, count, blocks, state=(x, *state), last=last)
        tiles.append(tile)
    row_parts = state[0]
    row_parts = lax.all_to_all(row_parts, PLANE_AXES, 0, 0, tiled=True)
    (col_parts,) = columns(where, row_parts, src_norm, tiles, True)
    col_parts = lax.all_to_all(col_parts, "z", 0, 0, tiled=True)
    row_parts = rows(where, col_parts, tiles)
    row_parts = lax.all_to_all(row_parts, PLANE_AXES, 0, 0, tiled=True)
    col_parts, source_pots = columns(where, row_parts, src_norm, tiles, False)
    col_parts = lax.all_to_all(col_parts, "z", 0, 0, tiled=True)
    target_pots = pl.pallas_call(
        finish_kernel, out_shape=jax.ShapeDtypeStruct((COLS // 128, 128), jnp.float32), name="finish"
    )(col_parts, dst_norm)
    return (source_pots.reshape(ROWS), target_pots.reshape(COLS))


def solution(mesh):
    finer = Mesh(mesh.devices.reshape(2, 8, 4, 2, 2), (*BLK, *TGT))
    return jax.shard_map(
        body,
        mesh=finer,
        in_specs=(P(BLK, None), P((*BLK, *TGT), None), P((*BLK, *TGT))),
        out_specs=(P(BLK), P((*BLK, *TGT))),
        check_vma=False,
    )
```

```python
import functools
import math

import jax
import jax.numpy as jnp
from jax import lax
from jax.experimental import pallas as pl
from jax.experimental.pallas import tpu as pltpu
from jax.sharding import Mesh
from jax.sharding import PartitionSpec as P


EPS = 0.05
SCALE = math.log2(math.e) / EPS
LOG2E = math.log2(math.e)
N_SRC = 16384
N_DST = 65536
ROWS = 1024
COLS = 256
RING = 8
PLANE = 16
LANES = 128
TILES = ROWS // LANES
MIB = 1024 * 1024

BLK = ("xl", "z")
TGT = ("y", "xh", "core")
PLANE_AXES = ("xl", "y", "xh")

VMEM = pl.BlockSpec(memory_space=pltpu.VMEM)


def log2(x):
    return jnp.log(x) * LOG2E


def diagonal():
    shape = (LANES, LANES)
    return lax.broadcasted_iota(jnp.int32, shape, 0) == lax.broadcasted_iota(jnp.int32, shape, 1)


def as_column(eye, row):
    return jnp.sum(jnp.where(eye, row, 0.0), axis=1, keepdims=True)


def as_row(eye, column):
    return jnp.sum(jnp.where(eye, column, 0.0), axis=0, keepdims=True)


def tree(op, parts):
    parts = list(parts)
    while len(parts) > 1:
        parts = [op(*parts[k : k + 2]) if k + 1 < len(parts) else parts[k] for k in range(0, len(parts), 2)]
    return parts[0]


def three_parts(x):
    high = x.astype(jnp.bfloat16)
    rest = x - high.astype(jnp.float32)
    mid = rest.astype(jnp.bfloat16)
    low = (rest - mid.astype(jnp.float32)).astype(jnp.bfloat16)
    return high, mid, low


def online(scores, state):
    high = tree(jnp.maximum, scores)
    if state is None:
        return high, tree(jnp.add, [jnp.exp2(s - high) for s in scores])
    high = jnp.maximum(high, state[0])
    total = tree(jnp.add, [jnp.exp2(s - high) for s in scores])
    return high, state[1] * jnp.exp2(state[0] - high) + total


def over_sublanes(high, total):
    top = jnp.max(high, axis=0, keepdims=True)
    return top + log2(jnp.sum(total * jnp.exp2(high - top), axis=0, keepdims=True))


def joined(parts):
    top = jnp.max(parts, axis=0)
    return top + log2(jnp.sum(jnp.exp2(parts - top[None]), axis=0))


def put_rows(rows_ref, state_of):
    for half in range(2):
        tiles = [slice(t * LANES, (t + 1) * LANES) for t in range(TILES)]
        lse = jnp.concatenate([over_sublanes(*state_of(half, tile)) for tile in tiles], axis=0)
        for peer in range(PLANE):
            rows_ref[peer, half] = lse


def prepare_sources(x, half, x_ref):
    turned = (x * (2.0 * SCALE)).T
    high, mid, low = three_parts(turned)
    for k, part in enumerate((high, high, mid, mid, low, high)):
        x_ref[half, k * LANES : (k + 1) * LANES, :] = part


def prepare_targets(eye, block_ref, pots_ref):
    y = block_ref[0:COLS, :]
    norms = jnp.sum(y * y, axis=1, keepdims=True)
    for c in range(COLS // LANES):
        rows = slice(c * LANES, (c + 1) * LANES)
        column = as_column(eye, block_ref[COLS + c : COLS + c + 1, :])
        pots_ref[rows, :] = jnp.broadcast_to((column - norms[rows]) * SCALE, (LANES, LANES))
    high, mid, low = three_parts(y)
    return jnp.concatenate([high, mid, high, mid, high, low], axis=1), norms


def add_block(parts, pots_ref, at, half, x_ref, tile_ref, state_ref, fresh):
    step = 512
    for n in range(ROWS // step):
        lanes = slice(n * step, (n + 1) * step)
        tile_ref[at, half, :, lanes] = jnp.dot(parts, x_ref[half, :, lanes], preferred_element_type=jnp.float32)
        for t in range(n * step // LANES, (n + 1) * step // LANES):
            tile = slice(t * LANES, (t + 1) * LANES)
            state = None if fresh else (state_ref[0, half, :, tile], state_ref[1, half, :, tile])
            for c in range(2):
                rows = range(c * LANES, (c + 1) * LANES, 8)
                state = online([tile_ref[at, half, r : r + 8, tile] + pots_ref[r : r + 8, :] for r in rows], state)
            state_ref[0, half, :, tile], state_ref[1, half, :, tile] = state


def start_kernel(sources_ref, block_ref, tile_ref, x_ref, state_ref, src_norm_ref, dst_norm_ref, pots_scr):
    z, mine = lax.axis_index("z"), lax.axis_index("xl")
    eye = diagonal()
    x = sources_ref[...]
    prepare_sources(x, mine, x_ref)
    squares = jnp.sum(x * x, axis=1, keepdims=True)
    for c in range(TILES):
        src_norm_ref[c : c + 1, :] = as_row(eye, squares[c * LANES : (c + 1) * LANES])
    parts, norms = prepare_targets(eye, block_ref, pots_scr)
    for c in range(COLS // LANES):
        dst_norm_ref[c : c + 1, :] = as_row(eye, norms[c * LANES : (c + 1) * LANES])
    add_block(parts, pots_scr, z, mine, x_ref, tile_ref, state_ref, True)


def second_kernel(sources_ref, own_ref, lower_ref, upper_ref, *refs):
    (tile_ref, x_ref, state_ref), pots_scr = refs[3:6], refs[6]
    z, mine = lax.axis_index("z"), lax.axis_index("xl")
    eye = diagonal()
    prepare_sources(sources_ref[...], 1 - mine, x_ref)
    for b, (block_ref, offset) in enumerate(((own_ref, 0), (lower_ref, -1), (upper_ref, 1))):
        parts, _ = prepare_targets(eye, block_ref, pots_scr.at[b])
        at = lax.rem(z + (offset + RING), RING)
        if offset:
            add_block(parts, pots_scr.at[b], at, mine, x_ref, tile_ref, state_ref, False)
        add_block(parts, pots_scr.at[b], at, 1 - mine, x_ref, tile_ref, state_ref, not offset)


def more_kernel(offsets, last, x_ref, *refs):
    count = len(offsets)
    blocks, (tile_ref, state_ref) = refs[:count], refs[count + 2 : count + 4]
    pots_scr = refs[-1]
    z = lax.axis_index("z")
    eye = diagonal()
    for b, offset in enumerate(offsets):
        parts, _ = prepare_targets(eye, blocks[b], pots_scr.at[b])
        at = lax.rem(z + (offset + RING), RING)
        for half in range(2):
            add_block(parts, pots_scr.at[b], at, half, x_ref, tile_ref, state_ref, False)
    if last:
        put_rows(refs[count + 4], lambda half, tile: (state_ref[0, half, :, tile], state_ref[1, half, :, tile]))


F32 = jnp.float32
TILE = jax.ShapeDtypeStruct((RING, 2, COLS, ROWS), F32)
PARTS = jax.ShapeDtypeStruct((2, 6 * LANES, ROWS), jnp.bfloat16)
STATE = jax.ShapeDtypeStruct((2, 2, 8, ROWS), F32)
ROW_LSE = jax.ShapeDtypeStruct((PLANE, 2, TILES, LANES), F32)


def call(kernel, args, outs, blocks, scratch=(), aliases={}):
    return pl.pallas_call(
        kernel,
        out_shape=outs,
        in_specs=[VMEM] * len(args),
        out_specs=[VMEM] * len(outs),
        scratch_shapes=list(scratch),
        input_output_aliases=aliases,
        compiler_params=pltpu.CompilerParams(vmem_limit_bytes=24 * MIB),
        cost_estimate=pl.CostEstimate(
            flops=blocks * 2 * COLS * ROWS * 768, bytes_accessed=MIB, transcendentals=blocks * COLS * ROWS
        ),
    )(*args)


def columns_kernel(copies, rows_ref, src_norm_ref, tile_ref, *refs):
    if copies:
        cols_ref, high_scr, total_scr, lse_scr = refs
    else:
        cols_ref, source_pots_ref, high_scr, total_scr, lse_scr = refs
    u = -math.log2(N_DST) - joined(rows_ref[...])
    if not copies:
        mine = lax.axis_index("xl")
        own = jnp.where(mine == 0, u[0], u[1])
        source_pots_ref[...] = own * (1.0 / SCALE) + src_norm_ref[...]
    pots = [jnp.broadcast_to(u[h, t : t + 1, :], (8, LANES)) for h in range(2) for t in range(TILES)]
    high_scr[...] = jnp.zeros_like(high_scr)
    total_scr[...] = jnp.ones_like(total_scr)

    def finish(k):
        for c in range(COLS // LANES):
            rows = slice(c * LANES, (c + 1) * LANES)
            high, total = high_scr[rows, :].T, total_scr[rows, :].T
            top = jnp.max(high, axis=0, keepdims=True)
            lse_scr[k, c : c + 1, :] = top + log2(jnp.sum(total * jnp.exp2(high - top), axis=0, keepdims=True))

    def block(k, carry):
        finish(jnp.maximum(k - 1, 0))
        for r in range(0, COLS, 8):
            scores = [
                tile_ref[k, h, r : r + 8, t * LANES : (t + 1) * LANES] + pots[h * TILES + t]
                for h in range(2)
                for t in range(TILES)
            ]
            high_scr[r : r + 8, :], total_scr[r : r + 8, :] = online(scores, None)
        return carry

    lax.fori_loop(0, RING, block, 0)
    finish(RING - 1)
    if copies:
        lse = lse_scr[...].reshape(RING * 2, LANES)
        for peer in range(RING):
            cols_ref[peer] = lse
    else:
        cols_ref[...] = lse_scr[...]


def columns(rows, src_norm, tile, copies):
    if copies:
        outs = [jax.ShapeDtypeStruct((RING, RING * 2, LANES), F32)]
    else:
        outs = [jax.ShapeDtypeStruct((RING, 2, LANES), F32), jax.ShapeDtypeStruct((TILES, LANES), F32)]
    scratch = [pltpu.VMEM((COLS, LANES), F32)] * 2 + [pltpu.VMEM((RING, 2, LANES), F32)]
    return call(functools.partial(columns_kernel, copies), (rows, src_norm, tile), outs, 16, scratch)


def rows_kernel(cols_ref, tile_ref, rows_ref, w_scr, pots_scr, high_scr, total_scr):
    eye = diagonal()
    w_scr[...] = (-math.log2(N_SRC) - joined(cols_ref[...])).reshape(RING, 2, LANES)
    high_scr[...] = jnp.full_like(high_scr, -3.0e38)
    total_scr[...] = jnp.zeros_like(total_scr)

    def spread(k, slot):
        for c in range(2):
            column = as_column(eye, w_scr[k, c : c + 1, :])
            pots_scr[slot, c * LANES : (c + 1) * LANES, :] = jnp.broadcast_to(column, (LANES, LANES))

    def block(k, slot):
        for half in range(2):
            for t in range(TILES):
                tile = slice(t * LANES, (t + 1) * LANES)
                state = high_scr[half, :, tile], total_scr[half, :, tile]
                for c in range(2):
                    rows = range(c * LANES, (c + 1) * LANES, 8)
                    scores = [tile_ref[k, half, r : r + 8, tile] + pots_scr[slot, r : r + 8, :] for r in rows]
                    state = online(scores, state)
                high_scr[half, :, tile], total_scr[half, :, tile] = state

    def two_blocks(i, carry):
        spread(2 * i + 1, 1)
        block(2 * i, 0)
        spread(jnp.minimum(2 * i + 2, RING - 1), 0)
        block(2 * i + 1, 1)
        return carry

    spread(0, 0)
    lax.fori_loop(0, RING // 2, two_blocks, 0)
    put_rows(rows_ref, lambda half, tile: (high_scr[half, :, tile], total_scr[half, :, tile]))


def rows(cols, tile):
    scratch = [
        pltpu.VMEM((RING, 2, LANES), F32),
        pltpu.VMEM((2, COLS, LANES), F32),
        pltpu.VMEM((2, 8, ROWS), F32),
        pltpu.VMEM((2, 8, ROWS), F32),
    ]
    return call(rows_kernel, (cols, tile), [ROW_LSE], 16, scratch)[0]


def shifted(x, axis, by):
    count = lax.axis_size(axis)
    return lax.ppermute(x, axis, [(i, (i + by) % count) for i in range(count)])


def over_plane(copies):
    return lax.all_gather(lax.all_to_all(copies, PLANE_AXES, 0, 0, tiled=True), "core", tiled=True)


def steps(sources, targets, duals_init):
    packed = jnp.concatenate([targets, jnp.pad(duals_init.reshape(2, LANES), ((0, 6), (0, 0)))], axis=0)
    others = shifted(sources, "xl", 1)
    up, down = [packed], [packed]
    for step in range(1, RING // 2 + 1):
        up.append(shifted(up[-1], "z", 1))
        if step < RING // 2:
            down.append(shifted(down[-1], "z", -1))
    pots = pltpu.VMEM((COLS, LANES), F32)
    norms = [jax.ShapeDtypeStruct((TILES, LANES), F32), jax.ShapeDtypeStruct((2, LANES), F32)]
    tile, x, state, src_norm, dst_norm = call(start_kernel, (sources, packed), [TILE, PARTS, STATE, *norms], 1, [pots])
    tile, x, state = call(
        second_kernel,
        (others, packed, up[1], down[1], tile, x, state),
        [TILE, PARTS, STATE],
        5,
        [pltpu.VMEM((3, COLS, LANES), F32)],
        {4: 0, 5: 1, 6: 2},
    )
    for step in (2, 3, 4):
        last = step == RING // 2
        blocks = (up[step],) if last else (up[step], down[step])
        offsets = (-step,) if last else (-step, step)
        tile, state, *row_lse = call(
            functools.partial(more_kernel, offsets, last),
            (x, *blocks, tile, state),
            [TILE, STATE] + [ROW_LSE] * last,
            2 * len(blocks),
            [pltpu.VMEM((2, COLS, LANES), F32)],
            {1 + len(blocks): 0, 2 + len(blocks): 1},
        )
    (col_lse,) = columns(over_plane(row_lse[0]), src_norm, tile, True)
    row_lse = rows(lax.all_to_all(col_lse, "z", 0, 0, tiled=True), tile)
    col_lse, source_pots = columns(over_plane(row_lse), src_norm, tile, False)
    col_lse = joined(lax.all_to_all(col_lse, "z", 0, 0, tiled=True))
    target_pots = (-math.log2(N_SRC) - col_lse) * (1.0 / SCALE) + dst_norm
    return (source_pots.reshape(ROWS), target_pots.reshape(COLS))


def solution(mesh):
    finer = Mesh(mesh.devices.reshape(2, 8, 4, 2, 2), (*BLK, *TGT))
    return jax.shard_map(
        steps,
        mesh=finer,
        in_specs=(P(BLK, None), P((*BLK, *TGT), None), P((*BLK, *TGT))),
        out_specs=(P(BLK), P((*BLK, *TGT))),
        check_vma=False,
    )
```

```python
import functools
import math

import jax
import jax.numpy as jnp
from jax import lax
from jax.experimental import pallas as pl
from jax.experimental.pallas import tpu as pltpu
from jax.sharding import Mesh
from jax.sharding import PartitionSpec as P


EPS = 0.05
SCALE = math.log2(math.e) / EPS
LOG2E = math.log2(math.e)
N_SRC = 16384
N_DST = 65536
ROWS = 1024
COLS = 256
RING = 8
PLANE = 32
LANES = 128
TILES = ROWS // LANES
MIB = 1024 * 1024

BLK = ("xl", "z")
TGT = ("y", "xh", "core")
PLANE_AXES = ("xl", "y", "xh", "core")

VMEM = pl.BlockSpec(memory_space=pltpu.VMEM)


def log2(x):
    return jnp.log(x) * LOG2E


def diagonal():
    shape = (LANES, LANES)
    return lax.broadcasted_iota(jnp.int32, shape, 0) == lax.broadcasted_iota(jnp.int32, shape, 1)


def as_column(eye, row):
    return jnp.sum(jnp.where(eye, row, 0.0), axis=1, keepdims=True)


def as_row(eye, column):
    return jnp.sum(jnp.where(eye, column, 0.0), axis=0, keepdims=True)


def tree(op, parts):
    parts = list(parts)
    while len(parts) > 1:
        parts = [op(*parts[k : k + 2]) if k + 1 < len(parts) else parts[k] for k in range(0, len(parts), 2)]
    return parts[0]


def three_parts(x):
    high = x.astype(jnp.bfloat16)
    rest = x - high.astype(jnp.float32)
    mid = rest.astype(jnp.bfloat16)
    low = (rest - mid.astype(jnp.float32)).astype(jnp.bfloat16)
    return high, mid, low


def online(scores, state):
    high = tree(jnp.maximum, scores)
    if state is None:
        return high, tree(jnp.add, [jnp.exp2(s - high) for s in scores])
    high = jnp.maximum(high, state[0])
    total = tree(jnp.add, [jnp.exp2(s - high) for s in scores])
    return high, state[1] * jnp.exp2(state[0] - high) + total


def over_sublanes(high, total):
    top = jnp.max(high, axis=0, keepdims=True)
    return top + log2(jnp.sum(total * jnp.exp2(high - top), axis=0, keepdims=True))


def joined(parts):
    top = jnp.max(parts, axis=0)
    return top + log2(jnp.sum(jnp.exp2(parts - top[None]), axis=0))


def put_rows(rows_ref, state_of):
    for half in range(2):
        tiles = [slice(t * LANES, (t + 1) * LANES) for t in range(TILES)]
        lse = jnp.concatenate([over_sublanes(*state_of(half, tile)) for tile in tiles], axis=0)
        for peer in range(PLANE):
            rows_ref[peer, half] = lse


def prepare_sources(x, half, x_ref):
    turned = (x * (2.0 * SCALE)).T
    high, mid, low = three_parts(turned)
    for k, part in enumerate((high, high, mid, mid, low, high)):
        x_ref[half, k * LANES : (k + 1) * LANES, :] = part


def prepare_targets(eye, block_ref, pots_ref):
    y = block_ref[0:COLS, :]
    norms = jnp.sum(y * y, axis=1, keepdims=True)
    for c in range(COLS // LANES):
        rows = slice(c * LANES, (c + 1) * LANES)
        column = as_column(eye, block_ref[COLS + c : COLS + c + 1, :])
        pots_ref[rows, :] = jnp.broadcast_to((column - norms[rows]) * SCALE, (LANES, LANES))
    high, mid, low = three_parts(y)
    return jnp.concatenate([high, mid, high, mid, high, low], axis=1), norms


def add_block(parts, pots_ref, at, half, x_ref, tile_ref, state_ref, fresh):
    step = 512
    for n in range(ROWS // step):
        lanes = slice(n * step, (n + 1) * step)
        tile_ref[at, half, :, lanes] = jnp.dot(parts, x_ref[half, :, lanes], preferred_element_type=jnp.float32)
        for t in range(n * step // LANES, (n + 1) * step // LANES):
            tile = slice(t * LANES, (t + 1) * LANES)
            state = None if fresh else (state_ref[0, half, :, tile], state_ref[1, half, :, tile])
            for c in range(2):
                rows = range(c * LANES, (c + 1) * LANES, 8)
                state = online([tile_ref[at, half, r : r + 8, tile] + pots_ref[r : r + 8, :] for r in rows], state)
            state_ref[0, half, :, tile], state_ref[1, half, :, tile] = state


def ring_index(z, offset):
    return lax.rem(z + (offset + RING), RING)


def start_kernel(sources_ref, block_ref, tile_ref, x_ref, state_ref, src_norm_ref, dst_norm_ref, pots_scr):
    z, mine = lax.axis_index("z"), lax.axis_index("xl")
    eye = diagonal()
    x = sources_ref[...]
    prepare_sources(x, mine, x_ref)
    squares = jnp.sum(x * x, axis=1, keepdims=True)
    for c in range(TILES):
        src_norm_ref[c : c + 1, :] = as_row(eye, squares[c * LANES : (c + 1) * LANES])
    parts, norms = prepare_targets(eye, block_ref, pots_scr)
    for c in range(COLS // LANES):
        dst_norm_ref[c : c + 1, :] = as_row(eye, norms[c * LANES : (c + 1) * LANES])
    add_block(parts, pots_scr, z, mine, x_ref, tile_ref, state_ref, True)


def own_kernel(offsets, x_ref, *refs):
    blocks, (tile_ref, state_ref), pots_scr = refs[: len(offsets)], refs[-3:-1], refs[-1]
    z, mine = lax.axis_index("z"), lax.axis_index("xl")
    eye = diagonal()
    for b, offset in enumerate(offsets):
        parts, _ = prepare_targets(eye, blocks[b], pots_scr.at[b])
        add_block(parts, pots_scr.at[b], ring_index(z, offset), mine, x_ref, tile_ref, state_ref, False)


def partner_kernel(fresh, work, *refs):
    refs = list(refs)
    sources_ref = refs.pop(0) if fresh else None
    blocks, (tile_ref, x_ref, state_ref), pots_scr = refs[: len(work)], refs[-4:-1], refs[-1]
    z, mine = lax.axis_index("z"), lax.axis_index("xl")
    eye = diagonal()
    if fresh:
        prepare_sources(sources_ref[...], 1 - mine, x_ref)
    for b, (offset, own, partner) in enumerate(work):
        parts, _ = prepare_targets(eye, blocks[b], pots_scr.at[b])
        at = ring_index(z, offset)
        if own:
            add_block(parts, pots_scr.at[b], at, mine, x_ref, tile_ref, state_ref, False)
        if partner:
            add_block(parts, pots_scr.at[b], at, 1 - mine, x_ref, tile_ref, state_ref, fresh and b == 0)


def last_kernel(offset, x_ref, block_ref, *refs):
    (tile_ref, state_ref, rows_ref), pots_scr = refs[-4:-1], refs[-1]
    parts, _ = prepare_targets(diagonal(), block_ref, pots_scr)
    for half in range(2):
        add_block(parts, pots_scr, ring_index(lax.axis_index("z"), offset), half, x_ref, tile_ref, state_ref, False)
    put_rows(rows_ref, lambda half, tile: (state_ref[0, half, :, tile], state_ref[1, half, :, tile]))


F32 = jnp.float32
TILE = jax.ShapeDtypeStruct((RING, 2, COLS, ROWS), F32)
PARTS = jax.ShapeDtypeStruct((2, 6 * LANES, ROWS), jnp.bfloat16)
STATE = jax.ShapeDtypeStruct((2, 2, 8, ROWS), F32)
ROW_LSE = jax.ShapeDtypeStruct((PLANE, 2, TILES, LANES), F32)


def call(kernel, args, outs, blocks, scratch=(), aliases={}):
    return pl.pallas_call(
        kernel,
        out_shape=outs,
        in_specs=[VMEM] * len(args),
        out_specs=[VMEM] * len(outs),
        scratch_shapes=list(scratch),
        input_output_aliases=aliases,
        compiler_params=pltpu.CompilerParams(vmem_limit_bytes=24 * MIB),
        cost_estimate=pl.CostEstimate(
            flops=blocks * 2 * COLS * ROWS * 768, bytes_accessed=MIB, transcendentals=blocks * COLS * ROWS
        ),
    )(*args)


def columns_kernel(copies, rows_ref, src_norm_ref, tile_ref, *refs):
    if copies:
        cols_ref, high_scr, total_scr, lse_scr = refs
    else:
        cols_ref, source_pots_ref, high_scr, total_scr, lse_scr = refs
    u = -math.log2(N_DST) - joined(rows_ref[...])
    if not copies:
        mine = lax.axis_index("xl")
        own = jnp.where(mine == 0, u[0], u[1])
        source_pots_ref[...] = own * (1.0 / SCALE) + src_norm_ref[...]
    pots = [jnp.broadcast_to(u[h, t : t + 1, :], (8, LANES)) for h in range(2) for t in range(TILES)]
    high_scr[...] = jnp.zeros_like(high_scr)
    total_scr[...] = jnp.ones_like(total_scr)

    def finish(k):
        for c in range(COLS // LANES):
            rows = slice(c * LANES, (c + 1) * LANES)
            high, total = high_scr[rows, :].T, total_scr[rows, :].T
            top = jnp.max(high, axis=0, keepdims=True)
            lse_scr[k, c : c + 1, :] = top + log2(jnp.sum(total * jnp.exp2(high - top), axis=0, keepdims=True))

    def block(k, carry):
        finish(jnp.maximum(k - 1, 0))
        for r in range(0, COLS, 8):
            scores = [
                tile_ref[k, h, r : r + 8, t * LANES : (t + 1) * LANES] + pots[h * TILES + t]
                for h in range(2)
                for t in range(TILES)
            ]
            high_scr[r : r + 8, :], total_scr[r : r + 8, :] = online(scores, None)
        return carry

    lax.fori_loop(0, RING, block, 0)
    finish(RING - 1)
    if copies:
        lse = lse_scr[...].reshape(RING * 2, LANES)
        for peer in range(RING):
            cols_ref[peer] = lse
    else:
        cols_ref[...] = lse_scr[...]


def columns(rows, src_norm, tile, copies):
    if copies:
        outs = [jax.ShapeDtypeStruct((RING, RING * 2, LANES), F32)]
    else:
        outs = [jax.ShapeDtypeStruct((RING, 2, LANES), F32), jax.ShapeDtypeStruct((TILES, LANES), F32)]
    scratch = [pltpu.VMEM((COLS, LANES), F32)] * 2 + [pltpu.VMEM((RING, 2, LANES), F32)]
    return call(functools.partial(columns_kernel, copies), (rows, src_norm, tile), outs, 16, scratch)


def rows_kernel(cols_ref, tile_ref, rows_ref, w_scr, pots_scr, high_scr, total_scr):
    eye = diagonal()
    w_scr[...] = (-math.log2(N_SRC) - joined(cols_ref[...])).reshape(RING, 2, LANES)
    high_scr[...] = jnp.full_like(high_scr, -3.0e38)
    total_scr[...] = jnp.zeros_like(total_scr)

    def spread(k, slot):
        for c in range(2):
            column = as_column(eye, w_scr[k, c : c + 1, :])
            pots_scr[slot, c * LANES : (c + 1) * LANES, :] = jnp.broadcast_to(column, (LANES, LANES))

    def block(k, slot):
        for half in range(2):
            for t in range(TILES):
                tile = slice(t * LANES, (t + 1) * LANES)
                state = high_scr[half, :, tile], total_scr[half, :, tile]
                for c in range(2):
                    rows = range(c * LANES, (c + 1) * LANES, 8)
                    scores = [tile_ref[k, half, r : r + 8, tile] + pots_scr[slot, r : r + 8, :] for r in rows]
                    state = online(scores, state)
                high_scr[half, :, tile], total_scr[half, :, tile] = state

    def two_blocks(i, carry):
        spread(2 * i + 1, 1)
        block(2 * i, 0)
        spread(jnp.minimum(2 * i + 2, RING - 1), 0)
        block(2 * i + 1, 1)
        return carry

    spread(0, 0)
    lax.fori_loop(0, RING // 2, two_blocks, 0)
    put_rows(rows_ref, lambda half, tile: (high_scr[half, :, tile], total_scr[half, :, tile]))


def rows(cols, tile):
    scratch = [
        pltpu.VMEM((RING, 2, LANES), F32),
        pltpu.VMEM((2, COLS, LANES), F32),
        pltpu.VMEM((2, 8, ROWS), F32),
        pltpu.VMEM((2, 8, ROWS), F32),
    ]
    return call(rows_kernel, (cols, tile), [ROW_LSE], 16, scratch)[0]


def shifted(x, axis, by):
    count = lax.axis_size(axis)
    return lax.ppermute(x, axis, [(i, (i + by) % count) for i in range(count)])


def over_plane(copies):
    return lax.all_to_all(copies, PLANE_AXES, 0, 0, tiled=True)


def steps(sources, targets, duals_init):
    packed = jnp.concatenate([targets, jnp.pad(duals_init.reshape(2, LANES), ((0, 6), (0, 0)))], axis=0)
    up, down = [packed], [packed]
    for step in range(1, RING // 2 + 1):
        up.append(shifted(up[-1], "z", 1))
        if step < RING // 2:
            down.append(shifted(down[-1], "z", -1))
    others = shifted(sources, "xl", 1)
    pots = pltpu.VMEM((COLS, LANES), F32)
    norms = [jax.ShapeDtypeStruct((TILES, LANES), F32), jax.ShapeDtypeStruct((2, LANES), F32)]
    tile, x, state, src_norm, dst_norm = call(start_kernel, (sources, packed), [TILE, PARTS, STATE, *norms], 1, [pots])
    tile, state = call(
        functools.partial(own_kernel, (-1, 1)),
        (x, up[1], down[1], tile, state),
        [TILE, STATE],
        2,
        [pltpu.VMEM((2, COLS, LANES), F32)],
        {3: 0, 4: 1},
    )
    tile, x, state = call(
        functools.partial(partner_kernel, True, ((0, 0, 1), (-1, 0, 1), (1, 0, 1), (-2, 1, 0), (2, 1, 0))),
        (others, packed, up[1], down[1], up[2], down[2], tile, x, state),
        [TILE, PARTS, STATE],
        5,
        [pltpu.VMEM((5, COLS, LANES), F32)],
        {6: 0, 7: 1, 8: 2},
    )
    tile, x, state = call(
        functools.partial(partner_kernel, False, ((-2, 0, 1), (2, 0, 1), (-3, 1, 1), (3, 1, 1))),
        (up[2], down[2], up[3], down[3], tile, x, state),
        [TILE, PARTS, STATE],
        6,
        [pltpu.VMEM((4, COLS, LANES), F32)],
        {4: 0, 5: 1, 6: 2},
    )
    tile, state, row_lse = call(
        functools.partial(last_kernel, -4), (x, up[4], tile, state), [TILE, STATE, ROW_LSE], 2, [pots], {2: 0, 3: 1}
    )
    (col_lse,) = columns(over_plane(row_lse), src_norm, tile, True)
    row_lse = rows(lax.all_to_all(col_lse, "z", 0, 0, tiled=True), tile)
    col_lse, source_pots = columns(over_plane(row_lse), src_norm, tile, False)
    col_lse = joined(lax.all_to_all(col_lse, "z", 0, 0, tiled=True))
    target_pots = (-math.log2(N_SRC) - col_lse) * (1.0 / SCALE) + dst_norm
    return (source_pots.reshape(ROWS), target_pots.reshape(COLS))


def solution(mesh):
    finer = Mesh(mesh.devices.reshape(2, 8, 4, 2, 2), (*BLK, *TGT))
    return jax.shard_map(
        steps,
        mesh=finer,
        in_specs=(P(BLK, None), P((*BLK, *TGT), None), P((*BLK, *TGT))),
        out_specs=(P(BLK), P((*BLK, *TGT))),
        check_vma=False,
    )
```

```python
import functools
import math

import jax
import jax.numpy as jnp
from jax import lax
from jax.experimental import pallas as pl
from jax.experimental.pallas import tpu as pltpu
from jax.sharding import Mesh
from jax.sharding import PartitionSpec as P


EPS = 0.05
SCALE = math.log2(math.e) / EPS
LOG2E = math.log2(math.e)
N_SRC = 16384
N_DST = 65536
ROWS = 1024
COLS = 256
RING = 8
PLANE = 32
LANES = 128
TILES = ROWS // LANES
MIB = 1024 * 1024

BLK = ("xl", "z")
TGT = ("y", "xh", "core")
PLANE_AXES = ("xl", "y", "xh", "core")

VMEM = pl.BlockSpec(memory_space=pltpu.VMEM)


def log2(x):
    return jnp.log(x) * LOG2E


def diagonal():
    shape = (LANES, LANES)
    return lax.broadcasted_iota(jnp.int32, shape, 0) == lax.broadcasted_iota(jnp.int32, shape, 1)


def as_column(eye, row):
    return jnp.sum(jnp.where(eye, row, 0.0), axis=1, keepdims=True)


def as_row(eye, column):
    return jnp.sum(jnp.where(eye, column, 0.0), axis=0, keepdims=True)


def tree(op, parts):
    parts = list(parts)
    while len(parts) > 1:
        parts = [op(*parts[k : k + 2]) if k + 1 < len(parts) else parts[k] for k in range(0, len(parts), 2)]
    return parts[0]


def three_parts(x):
    high = x.astype(jnp.bfloat16)
    rest = x - high.astype(jnp.float32)
    mid = rest.astype(jnp.bfloat16)
    low = (rest - mid.astype(jnp.float32)).astype(jnp.bfloat16)
    return high, mid, low


def online(scores, state):
    high = tree(jnp.maximum, scores)
    if state is None:
        return high, tree(jnp.add, [jnp.exp2(s - high) for s in scores])
    high = jnp.maximum(high, state[0])
    total = tree(jnp.add, [jnp.exp2(s - high) for s in scores])
    return high, state[1] * jnp.exp2(state[0] - high) + total


def over_sublanes(high, total):
    top = jnp.max(high, axis=0, keepdims=True)
    return top + log2(jnp.sum(total * jnp.exp2(high - top), axis=0, keepdims=True))


def joined(parts):
    top = jnp.max(parts, axis=0)
    return top + log2(jnp.sum(jnp.exp2(parts - top[None]), axis=0))


def put_rows(rows_ref, state_of):
    for half in range(2):
        tiles = [slice(t * LANES, (t + 1) * LANES) for t in range(TILES)]
        lse = jnp.concatenate([over_sublanes(*state_of(half, tile)) for tile in tiles], axis=0)
        for peer in range(PLANE):
            rows_ref[peer, half] = lse


def prepare_sources(x, half, x_ref):
    turned = (x * (2.0 * SCALE)).T
    high, mid, low = three_parts(turned)
    for k, part in enumerate((high, high, mid, mid, low, high)):
        x_ref[half, k * LANES : (k + 1) * LANES, :] = part


def prepare_targets(eye, block_ref, pots_ref):
    y = block_ref[0:COLS, :]
    norms = jnp.sum(y * y, axis=1, keepdims=True)
    for c in range(COLS // LANES):
        rows = slice(c * LANES, (c + 1) * LANES)
        column = as_column(eye, block_ref[COLS + c : COLS + c + 1, :])
        pots_ref[rows, :] = jnp.broadcast_to((column - norms[rows]) * SCALE, (LANES, LANES))
    high, mid, low = three_parts(y)
    return jnp.concatenate([high, mid, high, mid, high, low], axis=1), norms


def add_block(parts, pots_ref, at, half, x_ref, tile_ref, state_ref, fresh):
    step = 512
    for n in range(ROWS // step):
        lanes = slice(n * step, (n + 1) * step)
        tile_ref[at, half, :, lanes] = jnp.dot(parts, x_ref[half, :, lanes], preferred_element_type=jnp.float32)
        for t in range(n * step // LANES, (n + 1) * step // LANES):
            tile = slice(t * LANES, (t + 1) * LANES)
            state = None if fresh else (state_ref[0, half, :, tile], state_ref[1, half, :, tile])
            for c in range(2):
                rows = range(c * LANES, (c + 1) * LANES, 8)
                state = online([tile_ref[at, half, r : r + 8, tile] + pots_ref[r : r + 8, :] for r in rows], state)
            state_ref[0, half, :, tile], state_ref[1, half, :, tile] = state


def ring_index(z, offset):
    return lax.rem(z + (offset + RING), RING)


def start_kernel(sources_ref, block_ref, tile_ref, x_ref, state_ref, src_norm_ref, dst_norm_ref, pots_scr):
    z, mine = lax.axis_index("z"), lax.axis_index("xl")
    eye = diagonal()
    x = sources_ref[...]
    prepare_sources(x, mine, x_ref)
    squares = jnp.sum(x * x, axis=1, keepdims=True)
    for c in range(TILES):
        src_norm_ref[c : c + 1, :] = as_row(eye, squares[c * LANES : (c + 1) * LANES])
    parts, norms = prepare_targets(eye, block_ref, pots_scr)
    for c in range(COLS // LANES):
        dst_norm_ref[c : c + 1, :] = as_row(eye, norms[c * LANES : (c + 1) * LANES])
    add_block(parts, pots_scr, z, mine, x_ref, tile_ref, state_ref, True)


def own_kernel(offsets, x_ref, *refs):
    blocks, (tile_ref, state_ref), pots_scr = refs[: len(offsets)], refs[-3:-1], refs[-1]
    z, mine = lax.axis_index("z"), lax.axis_index("xl")
    eye = diagonal()
    for b, offset in enumerate(offsets):
        parts, _ = prepare_targets(eye, blocks[b], pots_scr.at[b])
        add_block(parts, pots_scr.at[b], ring_index(z, offset), mine, x_ref, tile_ref, state_ref, False)


def partner_kernel(fresh, work, *refs):
    refs = list(refs)
    sources_ref = refs.pop(0) if fresh else None
    blocks, (tile_ref, x_ref, state_ref), pots_scr = refs[: len(work)], refs[-4:-1], refs[-1]
    z, mine = lax.axis_index("z"), lax.axis_index("xl")
    eye = diagonal()
    if fresh:
        prepare_sources(sources_ref[...], 1 - mine, x_ref)
    for b, (offset, own, partner) in enumerate(work):
        parts, _ = prepare_targets(eye, blocks[b], pots_scr.at[b])
        at = ring_index(z, offset)
        if own:
            add_block(parts, pots_scr.at[b], at, mine, x_ref, tile_ref, state_ref, False)
        if partner:
            add_block(parts, pots_scr.at[b], at, 1 - mine, x_ref, tile_ref, state_ref, fresh and b == 0)


def last_kernel(offset, x_ref, block_ref, *refs):
    (tile_ref, state_ref, rows_ref), pots_scr = refs[-4:-1], refs[-1]
    parts, _ = prepare_targets(diagonal(), block_ref, pots_scr)
    for half in range(2):
        add_block(parts, pots_scr, ring_index(lax.axis_index("z"), offset), half, x_ref, tile_ref, state_ref, False)
    put_rows(rows_ref, lambda half, tile: (state_ref[0, half, :, tile], state_ref[1, half, :, tile]))


F32 = jnp.float32
TILE = jax.ShapeDtypeStruct((RING, 2, COLS, ROWS), F32)
PARTS = jax.ShapeDtypeStruct((2, 6 * LANES, ROWS), jnp.bfloat16)
STATE = jax.ShapeDtypeStruct((2, 2, 8, ROWS), F32)
ROW_LSE = jax.ShapeDtypeStruct((PLANE, 2, TILES, LANES), F32)


def call(kernel, args, outs, blocks, scratch=(), aliases={}):
    return pl.pallas_call(
        kernel,
        out_shape=outs,
        in_specs=[VMEM] * len(args),
        out_specs=[VMEM] * len(outs),
        scratch_shapes=list(scratch),
        input_output_aliases=aliases,
        compiler_params=pltpu.CompilerParams(vmem_limit_bytes=24 * MIB),
        cost_estimate=pl.CostEstimate(
            flops=blocks * 2 * COLS * ROWS * 768, bytes_accessed=MIB, transcendentals=blocks * COLS * ROWS
        ),
    )(*args)


def columns_kernel(copies, rows_ref, src_norm_ref, tile_ref, *refs):
    if copies:
        cols_ref, high_scr, total_scr, lse_scr = refs
    else:
        cols_ref, source_pots_ref, high_scr, total_scr, lse_scr = refs
    u = -math.log2(N_DST) - joined(rows_ref[...])
    if not copies:
        mine = lax.axis_index("xl")
        own = jnp.where(mine == 0, u[0], u[1])
        source_pots_ref[...] = own * (1.0 / SCALE) + src_norm_ref[...]
    pots = [jnp.broadcast_to(u[h, t : t + 1, :], (8, LANES)) for h in range(2) for t in range(TILES)]
    high_scr[...] = jnp.zeros_like(high_scr)
    total_scr[...] = jnp.ones_like(total_scr)

    def finish(k):
        for c in range(COLS // LANES):
            rows = slice(c * LANES, (c + 1) * LANES)
            highs = [high_scr[h, rows, :].T for h in range(2)]
            top = jnp.max(jnp.maximum(*highs), axis=0, keepdims=True)
            total = sum(total_scr[h, rows, :].T * jnp.exp2(highs[h] - top) for h in range(2))
            lse_scr[k, c : c + 1, :] = top + log2(jnp.sum(total, axis=0, keepdims=True))

    def block(k, carry):
        finish(jnp.maximum(k - 1, 0))
        for h in range(2):
            for r in range(0, COLS, 8):
                tiles = [slice(t * LANES, (t + 1) * LANES) for t in range(TILES)]
                scores = [tile_ref[k, h, r : r + 8, tiles[t]] + pots[h * TILES + t] for t in range(TILES)]
                high_scr[h, r : r + 8, :], total_scr[h, r : r + 8, :] = online(scores, None)
        return carry

    lax.fori_loop(0, RING, block, 0)
    finish(RING - 1)
    if copies:
        lse = lse_scr[...].reshape(RING * 2, LANES)
        for peer in range(RING):
            cols_ref[peer] = lse
    else:
        cols_ref[...] = lse_scr[...]


def columns(rows, src_norm, tile, copies):
    if copies:
        outs = [jax.ShapeDtypeStruct((RING, RING * 2, LANES), F32)]
    else:
        outs = [jax.ShapeDtypeStruct((RING, 2, LANES), F32), jax.ShapeDtypeStruct((TILES, LANES), F32)]
    scratch = [pltpu.VMEM((2, COLS, LANES), F32)] * 2 + [pltpu.VMEM((RING, 2, LANES), F32)]
    return call(functools.partial(columns_kernel, copies), (rows, src_norm, tile), outs, 16, scratch)


def rows_kernel(cols_ref, tile_ref, rows_ref, w_scr, pots_scr, high_scr, total_scr):
    eye = diagonal()
    w_scr[...] = (-math.log2(N_SRC) - joined(cols_ref[...])).reshape(RING, 2, LANES)
    high_scr[...] = jnp.full_like(high_scr, -3.0e38)
    total_scr[...] = jnp.zeros_like(total_scr)

    def spread(k, slot):
        for c in range(2):
            column = as_column(eye, w_scr[k, c : c + 1, :])
            pots_scr[slot, c * LANES : (c + 1) * LANES, :] = jnp.broadcast_to(column, (LANES, LANES))

    def block(k, slot):
        for half in range(2):
            for t in range(TILES):
                tile = slice(t * LANES, (t + 1) * LANES)
                state = high_scr[half, :, tile], total_scr[half, :, tile]
                for c in range(2):
                    rows = range(c * LANES, (c + 1) * LANES, 8)
                    scores = [tile_ref[k, half, r : r + 8, tile] + pots_scr[slot, r : r + 8, :] for r in rows]
                    state = online(scores, state)
                high_scr[half, :, tile], total_scr[half, :, tile] = state

    def two_blocks(i, carry):
        spread(2 * i + 1, 1)
        block(2 * i, 0)
        spread(jnp.minimum(2 * i + 2, RING - 1), 0)
        block(2 * i + 1, 1)
        return carry

    spread(0, 0)
    lax.fori_loop(0, RING // 2, two_blocks, 0)
    put_rows(rows_ref, lambda half, tile: (high_scr[half, :, tile], total_scr[half, :, tile]))


def rows(cols, tile):
    scratch = [
        pltpu.VMEM((RING, 2, LANES), F32),
        pltpu.VMEM((2, COLS, LANES), F32),
        pltpu.VMEM((2, 8, ROWS), F32),
        pltpu.VMEM((2, 8, ROWS), F32),
    ]
    return call(rows_kernel, (cols, tile), [ROW_LSE], 16, scratch)[0]


def shifted(x, axis, by):
    count = lax.axis_size(axis)
    return lax.ppermute(x, axis, [(i, (i + by) % count) for i in range(count)])


def over_plane(copies):
    return lax.all_to_all(copies, PLANE_AXES, 0, 0, tiled=True)


def steps(sources, targets, duals_init):
    packed = jnp.concatenate([targets, jnp.pad(duals_init.reshape(2, LANES), ((0, 6), (0, 0)))], axis=0)
    others = shifted(sources, "xl", 1)
    up, down = [packed], [packed]
    for step in range(1, RING // 2 + 1):
        up.append(shifted(up[-1], "z", 1))
        if step < RING // 2:
            down.append(shifted(down[-1], "z", -1))
    pots = pltpu.VMEM((COLS, LANES), F32)
    norms = [jax.ShapeDtypeStruct((TILES, LANES), F32), jax.ShapeDtypeStruct((2, LANES), F32)]
    tile, x, state, src_norm, dst_norm = call(start_kernel, (sources, packed), [TILE, PARTS, STATE, *norms], 1, [pots])

    def own(step):
        return call(
            functools.partial(own_kernel, (-step, step)),
            (x, up[step], down[step], tile, state),
            [TILE, STATE],
            2,
            [pltpu.VMEM((2, COLS, LANES), F32)],
            {3: 0, 4: 1},
        )

    def partner(fresh, work, *blocks):
        first = (others,) if fresh else ()
        at = len(first) + len(blocks)
        return call(
            functools.partial(partner_kernel, fresh, work),
            (*first, *blocks, tile, x, state),
            [TILE, PARTS, STATE],
            sum(a + b for _, a, b in work),
            [pltpu.VMEM((len(work), COLS, LANES), F32)],
            {at: 0, at + 1: 1, at + 2: 2},
        )

    tile, state = own(1)
    tile, state = own(2)
    tile, x, state = partner(True, ((0, 0, 1), (-1, 0, 1), (1, 0, 1)), packed, up[1], down[1])
    work = ((-2, 0, 1), (2, 0, 1), (-3, 1, 1), (3, 1, 1))
    tile, x, state = partner(False, work, up[2], down[2], up[3], down[3])
    tile, state, row_lse = call(
        functools.partial(last_kernel, -4), (x, up[4], tile, state), [TILE, STATE, ROW_LSE], 2, [pots], {2: 0, 3: 1}
    )
    (col_lse,) = columns(over_plane(row_lse), src_norm, tile, True)
    row_lse = rows(lax.all_to_all(col_lse, "z", 0, 0, tiled=True), tile)
    col_lse, source_pots = columns(over_plane(row_lse), src_norm, tile, False)
    col_lse = joined(lax.all_to_all(col_lse, "z", 0, 0, tiled=True))
    target_pots = (-math.log2(N_SRC) - col_lse) * (1.0 / SCALE) + dst_norm
    return (source_pots.reshape(ROWS), target_pots.reshape(COLS))


def solution(mesh):
    finer = Mesh(mesh.devices.reshape(2, 8, 4, 2, 2), (*BLK, *TGT))
    return jax.shard_map(
        steps,
        mesh=finer,
        in_specs=(P(BLK, None), P((*BLK, *TGT), None), P((*BLK, *TGT))),
        out_specs=(P(BLK), P((*BLK, *TGT))),
        check_vma=False,
    )
```

```python
import functools
import math

import jax
import jax.numpy as jnp
from jax import lax
from jax.experimental import pallas as pl
from jax.experimental.pallas import tpu as pltpu
from jax.sharding import Mesh
from jax.sharding import PartitionSpec as P


EPS = 0.05
SCALE = math.log2(math.e) / EPS
LOG2E = math.log2(math.e)
N_SRC = 16384
N_DST = 65536
ROWS = 1024
COLS = 256
RING = 8
PLANE = 32
LANES = 128
TILES = ROWS // LANES
MIB = 1024 * 1024

BLK = ("xl", "z")
TGT = ("y", "xh", "core")
PLANE_AXES = ("xl", "y", "xh", "core")

VMEM = pl.BlockSpec(memory_space=pltpu.VMEM)


def log2(x):
    return jnp.log(x) * LOG2E


def diagonal():
    shape = (LANES, LANES)
    return lax.broadcasted_iota(jnp.int32, shape, 0) == lax.broadcasted_iota(jnp.int32, shape, 1)


def as_column(eye, row):
    return jnp.sum(jnp.where(eye, row, 0.0), axis=1, keepdims=True)


def as_row(eye, column):
    return jnp.sum(jnp.where(eye, column, 0.0), axis=0, keepdims=True)


def tree(op, parts):
    parts = list(parts)
    while len(parts) > 1:
        parts = [op(*parts[k : k + 2]) if k + 1 < len(parts) else parts[k] for k in range(0, len(parts), 2)]
    return parts[0]


def three_parts(x):
    high = x.astype(jnp.bfloat16)
    rest = x - high.astype(jnp.float32)
    mid = rest.astype(jnp.bfloat16)
    low = (rest - mid.astype(jnp.float32)).astype(jnp.bfloat16)
    return high, mid, low


def online(scores, state):
    high = tree(jnp.maximum, scores)
    if state is None:
        return high, tree(jnp.add, [jnp.exp2(s - high) for s in scores])
    high = jnp.maximum(high, state[0])
    total = tree(jnp.add, [jnp.exp2(s - high) for s in scores])
    return high, state[1] * jnp.exp2(state[0] - high) + total


def over_sublanes(high, total):
    top = jnp.max(high, axis=0, keepdims=True)
    return top + log2(jnp.sum(total * jnp.exp2(high - top), axis=0, keepdims=True))


def joined(parts):
    top = jnp.max(parts, axis=0)
    return top + log2(jnp.sum(jnp.exp2(parts - top[None]), axis=0))


def put_rows(rows_ref, state_of):
    for half in range(2):
        tiles = [slice(t * LANES, (t + 1) * LANES) for t in range(TILES)]
        lse = jnp.concatenate([over_sublanes(*state_of(half, tile)) for tile in tiles], axis=0)
        for peer in range(PLANE):
            rows_ref[peer, half] = lse


def prepare_sources(x, half, x_ref):
    turned = (x * (2.0 * SCALE)).T
    high, mid, low = three_parts(turned)
    for k, part in enumerate((high, high, mid, mid, low, high)):
        x_ref[half, k * LANES : (k + 1) * LANES, :] = part


def prepare_targets(eye, block_ref, pots_ref):
    y = block_ref[0:COLS, :]
    norms = jnp.sum(y * y, axis=1, keepdims=True)
    for c in range(COLS // LANES):
        rows = slice(c * LANES, (c + 1) * LANES)
        column = as_column(eye, block_ref[COLS + c : COLS + c + 1, :])
        pots_ref[rows, :] = jnp.broadcast_to((column - norms[rows]) * SCALE, (LANES, LANES))
    high, mid, low = three_parts(y)
    return jnp.concatenate([high, mid, high, mid, high, low], axis=1), norms


def add_block(parts, pots_ref, at, half, x_ref, tile_ref, state_ref, fresh):
    step = 512
    for n in range(ROWS // step):
        lanes = slice(n * step, (n + 1) * step)
        tile_ref[at, half, :, lanes] = jnp.dot(parts, x_ref[half, :, lanes], preferred_element_type=jnp.float32)
        for t in range(n * step // LANES, (n + 1) * step // LANES):
            tile = slice(t * LANES, (t + 1) * LANES)
            state = None if fresh else (state_ref[0, half, :, tile], state_ref[1, half, :, tile])
            for c in range(2):
                rows = range(c * LANES, (c + 1) * LANES, 8)
                state = online([tile_ref[at, half, r : r + 8, tile] + pots_ref[r : r + 8, :] for r in rows], state)
            state_ref[0, half, :, tile], state_ref[1, half, :, tile] = state


def ring_index(z, offset):
    return lax.rem(z + jnp.where(lax.rem(z, 2) == 0, offset, -offset) + RING, RING)


def start_kernel(sources_ref, block_ref, tile_ref, x_ref, state_ref, src_norm_ref, dst_norm_ref, pots_scr):
    z, mine = lax.axis_index("z"), lax.axis_index("xl")
    eye = diagonal()
    x = sources_ref[...]
    prepare_sources(x, mine, x_ref)
    squares = jnp.sum(x * x, axis=1, keepdims=True)
    for c in range(TILES):
        src_norm_ref[c : c + 1, :] = as_row(eye, squares[c * LANES : (c + 1) * LANES])
    parts, norms = prepare_targets(eye, block_ref, pots_scr)
    for c in range(COLS // LANES):
        dst_norm_ref[c : c + 1, :] = as_row(eye, norms[c * LANES : (c + 1) * LANES])
    add_block(parts, pots_scr, z, mine, x_ref, tile_ref, state_ref, True)


def own_kernel(offsets, x_ref, *refs):
    blocks, (tile_ref, state_ref), pots_scr = refs[: len(offsets)], refs[-3:-1], refs[-1]
    z, mine = lax.axis_index("z"), lax.axis_index("xl")
    eye = diagonal()
    for b, offset in enumerate(offsets):
        parts, _ = prepare_targets(eye, blocks[b], pots_scr.at[b])
        add_block(parts, pots_scr.at[b], ring_index(z, offset), mine, x_ref, tile_ref, state_ref, False)


def partner_kernel(fresh, work, *refs):
    refs = list(refs)
    sources_ref = refs.pop(0) if fresh else None
    blocks, (tile_ref, x_ref, state_ref), pots_scr = refs[: len(work)], refs[-4:-1], refs[-1]
    z, mine = lax.axis_index("z"), lax.axis_index("xl")
    eye = diagonal()
    if fresh:
        prepare_sources(sources_ref[...], 1 - mine, x_ref)
    for b, (offset, own, partner) in enumerate(work):
        parts, _ = prepare_targets(eye, blocks[b], pots_scr.at[b])
        at = ring_index(z, offset)
        if own:
            add_block(parts, pots_scr.at[b], at, mine, x_ref, tile_ref, state_ref, False)
        if partner:
            add_block(parts, pots_scr.at[b], at, 1 - mine, x_ref, tile_ref, state_ref, fresh and b == 0)


def last_kernel(offset, x_ref, block_ref, *refs):
    (tile_ref, state_ref, rows_ref), pots_scr = refs[-4:-1], refs[-1]
    parts, _ = prepare_targets(diagonal(), block_ref, pots_scr)
    for half in range(2):
        add_block(parts, pots_scr, ring_index(lax.axis_index("z"), offset), half, x_ref, tile_ref, state_ref, False)
    put_rows(rows_ref, lambda half, tile: (state_ref[0, half, :, tile], state_ref[1, half, :, tile]))


F32 = jnp.float32
TILE = jax.ShapeDtypeStruct((RING, 2, COLS, ROWS), F32)
PARTS = jax.ShapeDtypeStruct((2, 6 * LANES, ROWS), jnp.bfloat16)
STATE = jax.ShapeDtypeStruct((2, 2, 8, ROWS), F32)
ROW_LSE = jax.ShapeDtypeStruct((PLANE, 2, TILES, LANES), F32)


def call(kernel, args, outs, blocks, scratch=(), aliases={}):
    return pl.pallas_call(
        kernel,
        out_shape=outs,
        in_specs=[VMEM] * len(args),
        out_specs=[VMEM] * len(outs),
        scratch_shapes=list(scratch),
        input_output_aliases=aliases,
        compiler_params=pltpu.CompilerParams(vmem_limit_bytes=24 * MIB),
        cost_estimate=pl.CostEstimate(
            flops=blocks * 2 * COLS * ROWS * 768, bytes_accessed=MIB, transcendentals=blocks * COLS * ROWS
        ),
    )(*args)


def pick_kernel(plus_ref, minus_ref, far_ref):
    odd = lax.rem(lax.axis_index("z") + lax.axis_index("core"), 2) == 1
    far_ref[...] = jnp.where(odd, plus_ref[...], minus_ref[...])


def from_afar(plus, minus):
    (block,) = call(pick_kernel, (plus, minus), [jax.ShapeDtypeStruct(plus.shape, F32)], 0)
    pairs = [(2 * z + c, 2 * ((z + (2, -2)[c]) % RING) + c) for z in range(RING) for c in range(2)]
    return lax.ppermute(block, ("z", "core"), pairs)


def columns_kernel(copies, rows_ref, src_norm_ref, tile_ref, *refs):
    if copies:
        cols_ref, high_scr, total_scr, lse_scr = refs
    else:
        cols_ref, source_pots_ref, high_scr, total_scr, lse_scr = refs
    u = -math.log2(N_DST) - joined(rows_ref[...])
    if not copies:
        mine = lax.axis_index("xl")
        own = jnp.where(mine == 0, u[0], u[1])
        source_pots_ref[...] = own * (1.0 / SCALE) + src_norm_ref[...]
    pots = [jnp.broadcast_to(u[h, t : t + 1, :], (8, LANES)) for h in range(2) for t in range(TILES)]
    high_scr[...] = jnp.zeros_like(high_scr)
    total_scr[...] = jnp.ones_like(total_scr)

    def finish(k):
        for c in range(COLS // LANES):
            rows = slice(c * LANES, (c + 1) * LANES)
            highs = [high_scr[h, rows, :].T for h in range(2)]
            top = jnp.max(jnp.maximum(*highs), axis=0, keepdims=True)
            total = sum(total_scr[h, rows, :].T * jnp.exp2(highs[h] - top) for h in range(2))
            lse_scr[k, c : c + 1, :] = top + log2(jnp.sum(total, axis=0, keepdims=True))

    def block(k, carry):
        finish(jnp.maximum(k - 1, 0))
        for h in range(2):
            for r in range(0, COLS, 8):
                tiles = [slice(t * LANES, (t + 1) * LANES) for t in range(TILES)]
                scores = [tile_ref[k, h, r : r + 8, tiles[t]] + pots[h * TILES + t] for t in range(TILES)]
                high_scr[h, r : r + 8, :], total_scr[h, r : r + 8, :] = online(scores, None)
        return carry

    lax.fori_loop(0, RING, block, 0)
    finish(RING - 1)
    if copies:
        lse = lse_scr[...].reshape(RING * 2, LANES)
        for peer in range(RING):
            cols_ref[peer] = lse
    else:
        cols_ref[...] = lse_scr[...]


def columns(rows, src_norm, tile, copies):
    if copies:
        outs = [jax.ShapeDtypeStruct((RING, RING * 2, LANES), F32)]
    else:
        outs = [jax.ShapeDtypeStruct((RING, 2, LANES), F32), jax.ShapeDtypeStruct((TILES, LANES), F32)]
    scratch = [pltpu.VMEM((2, COLS, LANES), F32)] * 2 + [pltpu.VMEM((RING, 2, LANES), F32)]
    return call(functools.partial(columns_kernel, copies), (rows, src_norm, tile), outs, 16, scratch)


def rows_kernel(cols_ref, tile_ref, rows_ref, w_scr, pots_scr, high_scr, total_scr):
    eye = diagonal()
    w_scr[...] = (-math.log2(N_SRC) - joined(cols_ref[...])).reshape(RING, 2, LANES)
    high_scr[...] = jnp.full_like(high_scr, -3.0e38)
    total_scr[...] = jnp.zeros_like(total_scr)

    def spread(k, slot):
        for c in range(2):
            column = as_column(eye, w_scr[k, c : c + 1, :])
            pots_scr[slot, c * LANES : (c + 1) * LANES, :] = jnp.broadcast_to(column, (LANES, LANES))

    def block(k, slot):
        for half in range(2):
            for t in range(TILES):
                tile = slice(t * LANES, (t + 1) * LANES)
                state = high_scr[half, :, tile], total_scr[half, :, tile]
                for c in range(2):
                    rows = range(c * LANES, (c + 1) * LANES, 8)
                    scores = [tile_ref[k, half, r : r + 8, tile] + pots_scr[slot, r : r + 8, :] for r in rows]
                    state = online(scores, state)
                high_scr[half, :, tile], total_scr[half, :, tile] = state

    def two_blocks(i, carry):
        spread(2 * i + 1, 1)
        block(2 * i, 0)
        spread(jnp.minimum(2 * i + 2, RING - 1), 0)
        block(2 * i + 1, 1)
        return carry

    spread(0, 0)
    lax.fori_loop(0, RING // 2, two_blocks, 0)
    put_rows(rows_ref, lambda half, tile: (high_scr[half, :, tile], total_scr[half, :, tile]))


def rows(cols, tile):
    scratch = [
        pltpu.VMEM((RING, 2, LANES), F32),
        pltpu.VMEM((2, COLS, LANES), F32),
        pltpu.VMEM((2, 8, ROWS), F32),
        pltpu.VMEM((2, 8, ROWS), F32),
    ]
    return call(rows_kernel, (cols, tile), [ROW_LSE], 16, scratch)[0]


def shifted(x, axis, by):
    count = lax.axis_size(axis)
    return lax.ppermute(x, axis, [(i, (i + by) % count) for i in range(count)])


def swapped(x, first):
    pairs = [(z, (z + (1 if z % 2 == first else -1)) % RING) for z in range(RING)]
    return lax.ppermute(x, "z", pairs)


def over_plane(copies):
    return lax.all_to_all(copies, PLANE_AXES, 0, 0, tiled=True)


def steps(sources, targets, duals_init):
    packed = jnp.concatenate([targets, jnp.pad(duals_init.reshape(2, LANES), ((0, 6), (0, 0)))], axis=0)
    plus, minus = [packed], [packed]
    for _ in range(1, RING // 2):
        from_pair = swapped(minus[-1], 0)
        minus.append(swapped(plus[-1], 1))
        plus.append(from_pair)
    far = from_afar(plus[2], minus[2])
    others = shifted(sources, "xl", 1)
    pots = pltpu.VMEM((COLS, LANES), F32)
    norms = [jax.ShapeDtypeStruct((TILES, LANES), F32), jax.ShapeDtypeStruct((2, LANES), F32)]
    tile, x, state, src_norm, dst_norm = call(start_kernel, (sources, packed), [TILE, PARTS, STATE, *norms], 1, [pots])

    def own(step):
        return call(
            functools.partial(own_kernel, (-step, step)),
            (x, minus[step], plus[step], tile, state),
            [TILE, STATE],
            2,
            [pltpu.VMEM((2, COLS, LANES), F32)],
            {3: 0, 4: 1},
        )

    def partner(fresh, work, *blocks):
        first = (others,) if fresh else ()
        at = len(first) + len(blocks)
        return call(
            functools.partial(partner_kernel, fresh, work),
            (*first, *blocks, tile, x, state),
            [TILE, PARTS, STATE],
            sum(a + b for _, a, b in work),
            [pltpu.VMEM((len(work), COLS, LANES), F32)],
            {at: 0, at + 1: 1, at + 2: 2},
        )

    tile, state = own(1)
    tile, state = own(2)
    work = tuple((offset, 0, 1) for offset in (0, -1, 1, -2, 2))
    tile, x, state = partner(True, work, packed, minus[1], plus[1], minus[2], plus[2])
    tile, x, state = partner(False, ((-3, 1, 1), (3, 1, 1)), minus[3], plus[3])
    tile, state, row_lse = call(
        functools.partial(last_kernel, -4), (x, far, tile, state), [TILE, STATE, ROW_LSE], 2, [pots], {2: 0, 3: 1}
    )
    (col_lse,) = columns(over_plane(row_lse), src_norm, tile, True)
    row_lse = rows(lax.all_to_all(col_lse, "z", 0, 0, tiled=True), tile)
    col_lse, source_pots = columns(over_plane(row_lse), src_norm, tile, False)
    col_lse = joined(lax.all_to_all(col_lse, "z", 0, 0, tiled=True))
    target_pots = (-math.log2(N_SRC) - col_lse) * (1.0 / SCALE) + dst_norm
    return (source_pots.reshape(ROWS), target_pots.reshape(COLS))


def solution(mesh):
    finer = Mesh(mesh.devices.reshape(2, 8, 4, 2, 2), (*BLK, *TGT))
    return jax.shard_map(
        steps,
        mesh=finer,
        in_specs=(P(BLK, None), P((*BLK, *TGT), None), P((*BLK, *TGT))),
        out_specs=(P(BLK), P((*BLK, *TGT))),
        check_vma=False,
    )
```

```python
import functools
import math

import jax
import jax.numpy as jnp
from jax import lax
from jax.experimental import pallas as pl
from jax.experimental.pallas import tpu as pltpu
from jax.sharding import Mesh
from jax.sharding import PartitionSpec as P


EPS = 0.05
SCALE = math.log2(math.e) / EPS
LOG2E = math.log2(math.e)
N_SRC = 16384
N_DST = 65536
ROWS = 1024
COLS = 256
RING = 8
PLANE = 32
LANES = 128
TILES = ROWS // LANES
MIB = 1024 * 1024

BLK = ("xl", "z")
TGT = ("y", "xh", "core")
PLANE_AXES = ("xl", "y", "xh", "core")

VMEM = pl.BlockSpec(memory_space=pltpu.VMEM)


def log2(x):
    return jnp.log(x) * LOG2E


def diagonal():
    shape = (LANES, LANES)
    return lax.broadcasted_iota(jnp.int32, shape, 0) == lax.broadcasted_iota(jnp.int32, shape, 1)


def as_column(eye, row):
    return jnp.sum(jnp.where(eye, row, 0.0), axis=1, keepdims=True)


def as_row(eye, column):
    return jnp.sum(jnp.where(eye, column, 0.0), axis=0, keepdims=True)


def tree(op, parts):
    parts = list(parts)
    while len(parts) > 1:
        parts = [op(*parts[k : k + 2]) if k + 1 < len(parts) else parts[k] for k in range(0, len(parts), 2)]
    return parts[0]


def three_parts(x):
    high = x.astype(jnp.bfloat16)
    rest = x - high.astype(jnp.float32)
    mid = rest.astype(jnp.bfloat16)
    low = (rest - mid.astype(jnp.float32)).astype(jnp.bfloat16)
    return high, mid, low


def online(scores, state):
    high = tree(jnp.maximum, scores)
    if state is None:
        return high, tree(jnp.add, [jnp.exp2(s - high) for s in scores])
    high = jnp.maximum(high, state[0])
    total = tree(jnp.add, [jnp.exp2(s - high) for s in scores])
    return high, state[1] * jnp.exp2(state[0] - high) + total


def over_sublanes(high, total):
    top = jnp.max(high, axis=0, keepdims=True)
    return top + log2(jnp.sum(total * jnp.exp2(high - top), axis=0, keepdims=True))


def joined(parts):
    top = jnp.max(parts, axis=0)
    return top + log2(jnp.sum(jnp.exp2(parts - top[None]), axis=0))


def put_rows(rows_ref, state_of):
    for half in range(2):
        lse = jnp.concatenate([over_sublanes(*state_of(half, t)) for t in range(TILES)], axis=0)
        for peer in range(PLANE):
            rows_ref[peer, half] = lse


def prepare_sources(x, half, x_ref):
    turned = (x * (2.0 * SCALE)).T
    high, mid, low = three_parts(turned)
    for k, part in enumerate((high, high, mid, mid, low, high)):
        x_ref[half, k * LANES : (k + 1) * LANES, :] = part


def prepare_targets(eye, block_ref, pots_ref):
    y = block_ref[0:COLS, :]
    norms = jnp.sum(y * y, axis=1, keepdims=True)
    for c in range(COLS // LANES):
        rows = slice(c * LANES, (c + 1) * LANES)
        column = as_column(eye, block_ref[COLS + c : COLS + c + 1, :])
        pots_ref[rows, :] = jnp.broadcast_to((column - norms[rows]) * SCALE, (LANES, LANES))
    high, mid, low = three_parts(y)
    return jnp.concatenate([high, mid, high, mid, high, low], axis=1), norms


def add_block(parts, pots_ref, at, half, x_ref, tile_ref, state_ref, fresh):
    step = 512
    for n in range(ROWS // step):
        lanes = slice(n * step, (n + 1) * step)
        tile_ref[at, half, :, lanes] = jnp.dot(parts, x_ref[half, :, lanes], preferred_element_type=jnp.float32)
        for t in range(n * step // LANES, (n + 1) * step // LANES):
            tile = slice(t * LANES, (t + 1) * LANES)
            state = None if fresh else (state_ref[0, half, :, tile], state_ref[1, half, :, tile])
            for c in range(0, COLS, 64):
                rows = range(c, c + 64, 8)
                state = online([tile_ref[at, half, r : r + 8, tile] + pots_ref[r : r + 8, :] for r in rows], state)
            state_ref[0, half, :, tile], state_ref[1, half, :, tile] = state


def ring_index(z, offset):
    return lax.rem(z + jnp.where(lax.rem(z, 2) == 0, offset, -offset) + RING, RING)


def start_kernel(sources_ref, block_ref, tile_ref, x_ref, state_ref, src_norm_ref, dst_norm_ref, pots_scr):
    z, mine = lax.axis_index("z"), lax.axis_index("xl")
    eye = diagonal()
    x = sources_ref[...]
    prepare_sources(x, mine, x_ref)
    squares = jnp.sum(x * x, axis=1, keepdims=True)
    for c in range(TILES):
        src_norm_ref[c : c + 1, :] = as_row(eye, squares[c * LANES : (c + 1) * LANES])
    parts, norms = prepare_targets(eye, block_ref, pots_scr)
    for c in range(COLS // LANES):
        dst_norm_ref[c : c + 1, :] = as_row(eye, norms[c * LANES : (c + 1) * LANES])
    add_block(parts, pots_scr, z, mine, x_ref, tile_ref, state_ref, True)


def own_kernel(offsets, x_ref, *refs):
    blocks, (tile_ref, state_ref), pots_scr = refs[: len(offsets)], refs[-3:-1], refs[-1]
    z, mine = lax.axis_index("z"), lax.axis_index("xl")
    eye = diagonal()
    for b, offset in enumerate(offsets):
        parts, _ = prepare_targets(eye, blocks[b], pots_scr.at[b])
        add_block(parts, pots_scr.at[b], ring_index(z, offset), mine, x_ref, tile_ref, state_ref, False)


def partner_kernel(fresh, work, *refs):
    refs = list(refs)
    sources_ref = refs.pop(0) if fresh else None
    blocks, (tile_ref, x_ref, state_ref), pots_scr = refs[: len(work)], refs[-4:-1], refs[-1]
    z, mine = lax.axis_index("z"), lax.axis_index("xl")
    eye = diagonal()
    if fresh:
        prepare_sources(sources_ref[...], 1 - mine, x_ref)
    for b, (offset, own, partner) in enumerate(work):
        parts, _ = prepare_targets(eye, blocks[b], pots_scr.at[b])
        at = ring_index(z, offset)
        if own:
            add_block(parts, pots_scr.at[b], at, mine, x_ref, tile_ref, state_ref, False)
        if partner:
            add_block(parts, pots_scr.at[b], at, 1 - mine, x_ref, tile_ref, state_ref, fresh and b == 0)


def last_kernel(offset, x_ref, block_ref, *refs):
    (tile_ref, state_ref, rows_ref), pots_scr = refs[-4:-1], refs[-1]
    parts, _ = prepare_targets(diagonal(), block_ref, pots_scr)
    for half in range(2):
        add_block(parts, pots_scr, ring_index(lax.axis_index("z"), offset), half, x_ref, tile_ref, state_ref, False)
    tiles = [slice(t * LANES, (t + 1) * LANES) for t in range(TILES)]
    put_rows(rows_ref, lambda half, t: (state_ref[0, half, :, tiles[t]], state_ref[1, half, :, tiles[t]]))


F32 = jnp.float32
TILE = jax.ShapeDtypeStruct((RING, 2, COLS, ROWS + LANES), F32)
PARTS = jax.ShapeDtypeStruct((2, 6 * LANES, ROWS), jnp.bfloat16)
STATE = jax.ShapeDtypeStruct((2, 2, 8, ROWS), F32)
ROW_LSE = jax.ShapeDtypeStruct((PLANE, 2, TILES, LANES), F32)


def call(kernel, args, outs, blocks, scratch=(), aliases={}):
    return pl.pallas_call(
        kernel,
        out_shape=outs,
        in_specs=[VMEM] * len(args),
        out_specs=[VMEM] * len(outs),
        scratch_shapes=list(scratch),
        input_output_aliases=aliases,
        compiler_params=pltpu.CompilerParams(vmem_limit_bytes=24 * MIB),
        cost_estimate=pl.CostEstimate(
            flops=blocks * 2 * COLS * ROWS * 768, bytes_accessed=MIB, transcendentals=blocks * COLS * ROWS
        ),
    )(*args)


def pick_kernel(plus_ref, minus_ref, far_ref):
    odd = lax.rem(lax.axis_index("z") + lax.axis_index("core"), 2) == 1
    far_ref[...] = jnp.where(odd, plus_ref[...], minus_ref[...])


def from_afar(plus, minus):
    (block,) = call(pick_kernel, (plus, minus), [jax.ShapeDtypeStruct(plus.shape, F32)], 0)
    pairs = [(2 * z + c, 2 * ((z + (2, -2)[c]) % RING) + c) for z in range(RING) for c in range(2)]
    return lax.ppermute(block, ("z", "core"), pairs)


def columns_kernel(copies, rows_ref, src_norm_ref, tile_ref, *refs):
    if copies:
        cols_ref, part_scr, turned_scr = refs
    else:
        cols_ref, source_pots_ref, part_scr, turned_scr = refs
    u = -math.log2(N_DST) - joined(rows_ref[...])
    if not copies:
        mine = lax.axis_index("xl")
        own = jnp.where(mine == 0, u[0], u[1])
        source_pots_ref[...] = own * (1.0 / SCALE) + src_norm_ref[...]
    pots = [jnp.broadcast_to(u[h, t : t + 1, :], (8, LANES)) for h in range(2) for t in range(TILES)]
    groups = 32
    turns = COLS // 8 // groups

    def load(i, g, h):
        k, first = i // turns, lax.rem(i, turns) * (8 * groups)
        rows = pl.ds(pl.multiple_of(first + 8 * g, 8), 8)
        scores = [tile_ref[k, h, rows, t * LANES : (t + 1) * LANES] + pots[h * TILES + t] for t in range(TILES)]
        return tree(jnp.maximum, scores), scores

    def turn(k, quarter):
        turned_scr[k, quarter] = part_scr[k, quarter].T

    def body(i, held):
        k, place = i // turns, lax.rem(i, turns)
        for quarter in range(4 // turns):
            turn(jnp.maximum(k - 1, 0), place * (4 // turns) + quarter)
        for g in range(groups):
            following = load(i, g, 1)
            high, scores = held
            total = tree(jnp.add, [jnp.exp2(s - high) for s in scores])
            held = following
            following = load(i, g + 1, 0) if g + 1 < groups else load(jnp.minimum(i + 1, RING * turns - 1), 0, 0)
            both, scores = jnp.maximum(high, held[0]), held[1]
            total = total * jnp.exp2(high - both) + tree(jnp.add, [jnp.exp2(s - both) for s in scores])
            half, rows = place + g // 16, slice(8 * (g % 16), 8 * (g % 16) + 8)
            part_scr[k, half, rows, :] = both
            part_scr[k, 2 + half, rows, :] = total
            held = following
        return held

    lax.fori_loop(0, RING * turns, body, load(0, 0, 0))
    for quarter in range(4):
        turn(RING - 1, quarter)
    for k in range(RING):
        for c in range(2):
            high = turned_scr[k, c]
            top = jnp.max(high, axis=0, keepdims=True)
            total = jnp.sum(turned_scr[k, 2 + c] * jnp.exp2(high - top), axis=0, keepdims=True)
            lse = top + log2(total)
            if copies:
                for peer in range(RING):
                    cols_ref[peer, 2 * k + c : 2 * k + c + 1, :] = lse
            else:
                cols_ref[k, c : c + 1, :] = lse


def columns(rows, src_norm, tile, copies):
    if copies:
        outs = [jax.ShapeDtypeStruct((RING, RING * 2, LANES), F32)]
    else:
        outs = [jax.ShapeDtypeStruct((RING, 2, LANES), F32), jax.ShapeDtypeStruct((TILES, LANES), F32)]
    scratch = [pltpu.VMEM((RING, 4, LANES, LANES), F32)] * 2
    return call(functools.partial(columns_kernel, copies), (rows, src_norm, tile), outs, 16, scratch)


def rows_kernel(cols_ref, tile_ref, rows_ref, w_scr, pots_scr, high_scr, total_scr):
    eye = diagonal()
    w = -math.log2(N_SRC) - joined(cols_ref[...])
    for r in range(2 * RING):
        w_scr[r] = w[r : r + 1, :]
    high_scr[...] = jnp.full_like(high_scr, -3.0e38)
    total_scr[...] = jnp.zeros_like(total_scr)
    unit = 8
    count = COLS // 8 // unit

    def spread(k):
        for c in range(2):
            pots_scr[k, c * LANES : (c + 1) * LANES, :] = jnp.broadcast_to(as_column(eye, w_scr[2 * k + c]), (LANES, LANES))

    def load(k, tile, part):
        half, t = divmod(tile, TILES)
        lanes = slice(t * LANES, (t + 1) * LANES)
        rows = [slice(8 * r, 8 * r + 8) for r in range(part * unit, (part + 1) * unit)]
        scores = [tile_ref[k, half, r, lanes] + pots_scr[k, r, :] for r in rows]
        return tree(jnp.maximum, scores), scores

    def body(k, held):
        for tile in range(2 * TILES):
            before, total = high_scr[tile], total_scr[tile]
            for part in range(count):
                if part + 1 < count:
                    following = load(k, tile, part + 1)
                elif tile + 1 < 2 * TILES:
                    following = load(k, tile + 1, 0)
                else:
                    following = load(jnp.minimum(k + 1, RING - 1), 0, 0)
                high, scores = jnp.maximum(held[0], before), held[1]
                total = total * jnp.exp2(before - high) + tree(jnp.add, [jnp.exp2(s - high) for s in scores])
                before, held = high, following
            high_scr[tile], total_scr[tile] = before, total
        spread(jnp.minimum(k + 2, RING - 1))
        return held

    spread(0)
    spread(1)
    lax.fori_loop(0, RING, body, load(0, 0, 0))
    put_rows(rows_ref, lambda half, tile: (high_scr[half * TILES + tile], total_scr[half * TILES + tile]))


def rows(cols, tile):
    scratch = [
        pltpu.VMEM((2 * RING, 1, LANES), F32),
        pltpu.VMEM((RING, COLS, LANES), F32),
        pltpu.VMEM((2 * TILES, 8, LANES), F32),
        pltpu.VMEM((2 * TILES, 8, LANES), F32),
    ]
    return call(rows_kernel, (cols, tile), [ROW_LSE], 16, scratch)[0]


def shifted(x, axis, by):
    count = lax.axis_size(axis)
    return lax.ppermute(x, axis, [(i, (i + by) % count) for i in range(count)])


def swapped(x, first):
    pairs = [(z, (z + (1 if z % 2 == first else -1)) % RING) for z in range(RING)]
    return lax.ppermute(x, "z", pairs)


def over_plane(copies):
    return lax.all_to_all(copies, PLANE_AXES, 0, 0, tiled=True)


def steps(sources, targets, duals_init):
    packed = jnp.concatenate([targets, jnp.pad(duals_init.reshape(2, LANES), ((0, 6), (0, 0)))], axis=0)
    plus, minus = [packed], [packed]
    for _ in range(1, RING // 2):
        from_pair = swapped(minus[-1], 0)
        minus.append(swapped(plus[-1], 1))
        plus.append(from_pair)
    far = from_afar(plus[2], minus[2])
    others = shifted(sources, "xl", 1)
    pots = pltpu.VMEM((COLS, LANES), F32)
    norms = [jax.ShapeDtypeStruct((TILES, LANES), F32), jax.ShapeDtypeStruct((2, LANES), F32)]
    tile, x, state, src_norm, dst_norm = call(start_kernel, (sources, packed), [TILE, PARTS, STATE, *norms], 1, [pots])

    def own(step):
        return call(
            functools.partial(own_kernel, (-step, step)),
            (x, minus[step], plus[step], tile, state),
            [TILE, STATE],
            2,
            [pltpu.VMEM((2, COLS, LANES), F32)],
            {3: 0, 4: 1},
        )

    def partner(fresh, work, *blocks):
        first = (others,) if fresh else ()
        at = len(first) + len(blocks)
        return call(
            functools.partial(partner_kernel, fresh, work),
            (*first, *blocks, tile, x, state),
            [TILE, PARTS, STATE],
            sum(a + b for _, a, b in work),
            [pltpu.VMEM((len(work), COLS, LANES), F32)],
            {at: 0, at + 1: 1, at + 2: 2},
        )

    tile, state = own(1)
    tile, state = own(2)
    work = tuple((offset, 0, 1) for offset in (0, -1, 1, -2, 2))
    tile, x, state = partner(True, work, packed, minus[1], plus[1], minus[2], plus[2])
    tile, x, state = partner(False, ((-3, 1, 1), (3, 1, 1)), minus[3], plus[3])
    tile, state, row_lse = call(
        functools.partial(last_kernel, -4), (x, far, tile, state), [TILE, STATE, ROW_LSE], 2, [pots], {2: 0, 3: 1}
    )
    (col_lse,) = columns(over_plane(row_lse), src_norm, tile, True)
    row_lse = rows(lax.all_to_all(col_lse, "z", 0, 0, tiled=True), tile)
    col_lse, source_pots = columns(over_plane(row_lse), src_norm, tile, False)
    col_lse = joined(lax.all_to_all(col_lse, "z", 0, 0, tiled=True))
    target_pots = (-math.log2(N_SRC) - col_lse) * (1.0 / SCALE) + dst_norm
    return (source_pots.reshape(ROWS), target_pots.reshape(COLS))


def solution(mesh):
    finer = Mesh(mesh.devices.reshape(2, 8, 4, 2, 2), (*BLK, *TGT))
    return jax.shard_map(
        steps,
        mesh=finer,
        in_specs=(P(BLK, None), P((*BLK, *TGT), None), P((*BLK, *TGT))),
        out_specs=(P(BLK), P((*BLK, *TGT))),
        check_vma=False,
    )
```

```python
import functools
import math

import jax
import jax.numpy as jnp
from jax import lax
from jax.experimental import pallas as pl
from jax.experimental.pallas import tpu as pltpu
from jax.sharding import Mesh
from jax.sharding import PartitionSpec as P


EPS = 0.05
SCALE = math.log2(math.e) / EPS
LOG2E = math.log2(math.e)
N_SRC = 16384
N_DST = 65536
ROWS = 1024
COLS = 256
RING = 8
PLANE = 32
LANES = 128
TILES = ROWS // LANES
MIB = 1024 * 1024

BLK = ("xl", "z")
TGT = ("y", "xh", "core")
PLANE_AXES = ("xl", "y", "xh", "core")

VMEM = pl.BlockSpec(memory_space=pltpu.VMEM)


def log2(x):
    return jnp.log(x) * LOG2E


def diagonal():
    shape = (LANES, LANES)
    return lax.broadcasted_iota(jnp.int32, shape, 0) == lax.broadcasted_iota(jnp.int32, shape, 1)


def as_column(eye, row):
    return jnp.sum(jnp.where(eye, row, 0.0), axis=1, keepdims=True)


def as_row(eye, column):
    return jnp.sum(jnp.where(eye, column, 0.0), axis=0, keepdims=True)


def tree(op, parts):
    parts = list(parts)
    while len(parts) > 1:
        parts = [op(*parts[k : k + 2]) if k + 1 < len(parts) else parts[k] for k in range(0, len(parts), 2)]
    return parts[0]


def three_parts(x):
    high = x.astype(jnp.bfloat16)
    rest = x - high.astype(jnp.float32)
    mid = rest.astype(jnp.bfloat16)
    low = (rest - mid.astype(jnp.float32)).astype(jnp.bfloat16)
    return high, mid, low


def online(scores, state):
    high = tree(jnp.maximum, scores)
    if state is None:
        return high, tree(jnp.add, [jnp.exp2(s - high) for s in scores])
    high = jnp.maximum(high, state[0])
    total = tree(jnp.add, [jnp.exp2(s - high) for s in scores])
    return high, state[1] * jnp.exp2(state[0] - high) + total


def over_sublanes(high, total):
    top = jnp.max(high, axis=0, keepdims=True)
    return top + log2(jnp.sum(total * jnp.exp2(high - top), axis=0, keepdims=True))


def joined(parts):
    top = jnp.max(parts, axis=0)
    return top + log2(jnp.sum(jnp.exp2(parts - top[None]), axis=0))


def put_rows(rows_ref, state_of):
    for half in range(2):
        lse = jnp.concatenate([over_sublanes(*state_of(half, t)) for t in range(TILES)], axis=0)
        for peer in range(PLANE):
            rows_ref[peer, half] = lse


def prepare_sources(x, half, x_ref):
    turned = (x * (2.0 * SCALE)).T
    high, mid, low = three_parts(turned)
    for k, part in enumerate((high, high, mid, mid, low, high)):
        x_ref[half, k * LANES : (k + 1) * LANES, :] = part


def prepare_targets(eye, block_ref, pots_ref):
    y = block_ref[0:COLS, :]
    norms = jnp.sum(y * y, axis=1, keepdims=True)
    for c in range(COLS // LANES):
        rows = slice(c * LANES, (c + 1) * LANES)
        column = as_column(eye, block_ref[COLS + c : COLS + c + 1, :])
        pots_ref[rows, :] = jnp.broadcast_to((column - norms[rows]) * SCALE, (LANES, LANES))
    high, mid, low = three_parts(y)
    return jnp.concatenate([high, mid, high, mid, high, low], axis=1), norms


def add_block(parts, pots_ref, at, half, x_ref, tile_ref, state_ref, fresh):
    step = 512
    for n in range(ROWS // step):
        lanes = slice(n * step, (n + 1) * step)
        tile_ref[at, half, :, lanes] = jnp.dot(parts, x_ref[half, :, lanes], preferred_element_type=jnp.float32)
        for t in range(n * step // LANES, (n + 1) * step // LANES):
            tile = slice(t * LANES, (t + 1) * LANES)
            state = None if fresh else (state_ref[0, half, :, tile], state_ref[1, half, :, tile])
            for c in range(0, COLS, 64):
                rows = range(c, c + 64, 8)
                state = online([tile_ref[at, half, r : r + 8, tile] + pots_ref[r : r + 8, :] for r in rows], state)
            state_ref[0, half, :, tile], state_ref[1, half, :, tile] = state


def ring_index(z, offset):
    return lax.rem(z + jnp.where(lax.rem(z, 2) == 0, offset, -offset) + RING, RING)


def start_kernel(sources_ref, block_ref, tile_ref, x_ref, state_ref, src_norm_ref, dst_norm_ref, pots_scr):
    z, mine = lax.axis_index("z"), lax.axis_index("xl")
    eye = diagonal()
    x = sources_ref[...]
    prepare_sources(x, mine, x_ref)
    squares = jnp.sum(x * x, axis=1, keepdims=True)
    for c in range(TILES):
        src_norm_ref[c : c + 1, :] = as_row(eye, squares[c * LANES : (c + 1) * LANES])
    parts, norms = prepare_targets(eye, block_ref, pots_scr)
    for c in range(COLS // LANES):
        dst_norm_ref[c : c + 1, :] = as_row(eye, norms[c * LANES : (c + 1) * LANES])
    add_block(parts, pots_scr, z, mine, x_ref, tile_ref, state_ref, True)


def own_kernel(offsets, x_ref, *refs):
    blocks, (tile_ref, state_ref), pots_scr = refs[: len(offsets)], refs[-3:-1], refs[-1]
    z, mine = lax.axis_index("z"), lax.axis_index("xl")
    eye = diagonal()
    for b, offset in enumerate(offsets):
        parts, _ = prepare_targets(eye, blocks[b], pots_scr.at[b])
        add_block(parts, pots_scr.at[b], ring_index(z, offset), mine, x_ref, tile_ref, state_ref, False)


def partner_kernel(fresh, work, *refs):
    refs = list(refs)
    sources_ref = refs.pop(0) if fresh else None
    blocks, (tile_ref, x_ref, state_ref), pots_scr = refs[: len(work)], refs[-4:-1], refs[-1]
    z, mine = lax.axis_index("z"), lax.axis_index("xl")
    eye = diagonal()
    if fresh:
        prepare_sources(sources_ref[...], 1 - mine, x_ref)
    for b, (offset, own, partner) in enumerate(work):
        parts, _ = prepare_targets(eye, blocks[b], pots_scr.at[b])
        at = ring_index(z, offset)
        if own:
            add_block(parts, pots_scr.at[b], at, mine, x_ref, tile_ref, state_ref, False)
        if partner:
            add_block(parts, pots_scr.at[b], at, 1 - mine, x_ref, tile_ref, state_ref, fresh and b == 0)


def last_kernel(offset, x_ref, block_ref, *refs):
    (tile_ref, state_ref, rows_ref), pots_scr = refs[-4:-1], refs[-1]
    parts, _ = prepare_targets(diagonal(), block_ref, pots_scr)
    for half in range(2):
        add_block(parts, pots_scr, ring_index(lax.axis_index("z"), offset), half, x_ref, tile_ref, state_ref, False)
    tiles = [slice(t * LANES, (t + 1) * LANES) for t in range(TILES)]
    put_rows(rows_ref, lambda half, t: (state_ref[0, half, :, tiles[t]], state_ref[1, half, :, tiles[t]]))


F32 = jnp.float32
TILE = jax.ShapeDtypeStruct((RING, 2, COLS, ROWS), F32)
PARTS = jax.ShapeDtypeStruct((2, 6 * LANES, ROWS), jnp.bfloat16)
STATE = jax.ShapeDtypeStruct((2, 2, 8, ROWS), F32)
ROW_LSE = jax.ShapeDtypeStruct((PLANE, 2, TILES, LANES), F32)


def call(kernel, args, outs, blocks, scratch=(), aliases={}):
    return pl.pallas_call(
        kernel,
        out_shape=outs,
        in_specs=[VMEM] * len(args),
        out_specs=[VMEM] * len(outs),
        scratch_shapes=list(scratch),
        input_output_aliases=aliases,
        compiler_params=pltpu.CompilerParams(vmem_limit_bytes=24 * MIB),
        cost_estimate=pl.CostEstimate(
            flops=blocks * 2 * COLS * ROWS * 768, bytes_accessed=MIB, transcendentals=blocks * COLS * ROWS
        ),
    )(*args)


def pick_kernel(plus_ref, minus_ref, far_ref):
    odd = lax.rem(lax.axis_index("z") + lax.axis_index("core"), 2) == 1
    far_ref[...] = jnp.where(odd, plus_ref[...], minus_ref[...])


def from_afar(plus, minus):
    (block,) = call(pick_kernel, (plus, minus), [jax.ShapeDtypeStruct(plus.shape, F32)], 0)
    pairs = [(2 * z + c, 2 * ((z + (2, -2)[c]) % RING) + c) for z in range(RING) for c in range(2)]
    return lax.ppermute(block, ("z", "core"), pairs)


def columns_kernel(copies, rows_ref, src_norm_ref, tile_ref, *refs):
    if copies:
        cols_ref, part_scr, turned_scr = refs
    else:
        cols_ref, source_pots_ref, part_scr, turned_scr = refs
    u = -math.log2(N_DST) - joined(rows_ref[...])
    if not copies:
        mine = lax.axis_index("xl")
        own = jnp.where(mine == 0, u[0], u[1])
        source_pots_ref[...] = own * (1.0 / SCALE) + src_norm_ref[...]
    pots = [jnp.broadcast_to(u[h, t : t + 1, :], (8, LANES)) for h in range(2) for t in range(TILES)]
    groups = 32
    turns = COLS // 8 // groups

    def load(i, g, h):
        k, first = i // turns, lax.rem(i, turns) * (8 * groups)
        rows = pl.ds(pl.multiple_of(first + 8 * g, 8), 8)
        scores = [tile_ref[k, h, rows, t * LANES : (t + 1) * LANES] + pots[h * TILES + t] for t in range(TILES)]
        return tree(jnp.maximum, scores), scores

    def turn(k, quarter):
        turned_scr[k, quarter] = part_scr[k, quarter].T

    def body(i, held):
        k, place = i // turns, lax.rem(i, turns)
        for quarter in range(4 // turns):
            turn(jnp.maximum(k - 1, 0), place * (4 // turns) + quarter)
        for g in range(groups):
            following = load(i, g, 1)
            high, scores = held
            total = tree(jnp.add, [jnp.exp2(s - high) for s in scores])
            held = following
            following = load(i, g + 1, 0) if g + 1 < groups else load(jnp.minimum(i + 1, RING * turns - 1), 0, 0)
            both, scores = jnp.maximum(high, held[0]), held[1]
            total = total * jnp.exp2(high - both) + tree(jnp.add, [jnp.exp2(s - both) for s in scores])
            half, rows = place + g // 16, slice(8 * (g % 16), 8 * (g % 16) + 8)
            part_scr[k, half, rows, :] = both
            part_scr[k, 2 + half, rows, :] = total
            held = following
        return held

    lax.fori_loop(0, RING * turns, body, load(0, 0, 0))
    for quarter in range(4):
        turn(RING - 1, quarter)
    for k in range(RING):
        for c in range(2):
            high = turned_scr[k, c]
            top = jnp.max(high, axis=0, keepdims=True)
            total = jnp.sum(turned_scr[k, 2 + c] * jnp.exp2(high - top), axis=0, keepdims=True)
            lse = top + log2(total)
            if copies:
                for peer in range(RING):
                    cols_ref[peer, 2 * k + c : 2 * k + c + 1, :] = lse
            else:
                cols_ref[k, c : c + 1, :] = lse


def columns(rows, src_norm, tile, copies):
    if copies:
        outs = [jax.ShapeDtypeStruct((RING, RING * 2, LANES), F32)]
    else:
        outs = [jax.ShapeDtypeStruct((RING, 2, LANES), F32), jax.ShapeDtypeStruct((TILES, LANES), F32)]
    scratch = [pltpu.VMEM((RING, 4, LANES, LANES), F32)] * 2
    return call(functools.partial(columns_kernel, copies), (rows, src_norm, tile), outs, 16, scratch)


def rows_kernel(cols_ref, tile_ref, rows_ref, w_scr, pots_scr, high_scr, total_scr):
    eye = diagonal()
    w_scr[...] = (-math.log2(N_SRC) - joined(cols_ref[...])).reshape(RING, 2, LANES)
    high_scr[...] = jnp.full_like(high_scr, -3.0e38)
    total_scr[...] = jnp.zeros_like(total_scr)

    def spread(k, slot):
        for c in range(2):
            column = as_column(eye, w_scr[k, c : c + 1, :])
            pots_scr[slot, c * LANES : (c + 1) * LANES, :] = jnp.broadcast_to(column, (LANES, LANES))

    def block(k, slot):
        for half in range(2):
            for t in range(TILES):
                tile = slice(t * LANES, (t + 1) * LANES)
                state = high_scr[half, :, tile], total_scr[half, :, tile]
                for c in range(0, COLS, 64):
                    rows = range(c, c + 64, 8)
                    scores = [tile_ref[k, half, r : r + 8, tile] + pots_scr[slot, r : r + 8, :] for r in rows]
                    state = online(scores, state)
                high_scr[half, :, tile], total_scr[half, :, tile] = state

    def two_blocks(i, carry):
        spread(2 * i + 1, 1)
        block(2 * i, 0)
        spread(jnp.minimum(2 * i + 2, RING - 1), 0)
        block(2 * i + 1, 1)
        return carry

    spread(0, 0)
    lax.fori_loop(0, RING // 2, two_blocks, 0)
    tiles = [slice(t * LANES, (t + 1) * LANES) for t in range(TILES)]
    put_rows(rows_ref, lambda half, t: (high_scr[half, :, tiles[t]], total_scr[half, :, tiles[t]]))


def rows(cols, tile):
    scratch = [
        pltpu.VMEM((RING, 2, LANES), F32),
        pltpu.VMEM((2, COLS, LANES), F32),
        pltpu.VMEM((2, 8, ROWS), F32),
        pltpu.VMEM((2, 8, ROWS), F32),
    ]
    return call(rows_kernel, (cols, tile), [ROW_LSE], 16, scratch)[0]


def shifted(x, axis, by):
    count = lax.axis_size(axis)
    return lax.ppermute(x, axis, [(i, (i + by) % count) for i in range(count)])


def swapped(x, first):
    pairs = [(z, (z + (1 if z % 2 == first else -1)) % RING) for z in range(RING)]
    return lax.ppermute(x, "z", pairs)


def over_plane(copies):
    return lax.all_to_all(copies, PLANE_AXES, 0, 0, tiled=True)


def steps(sources, targets, duals_init):
    packed = jnp.concatenate([targets, jnp.pad(duals_init.reshape(2, LANES), ((0, 6), (0, 0)))], axis=0)
    plus, minus = [packed], [packed]
    for _ in range(1, RING // 2):
        from_pair = swapped(minus[-1], 0)
        minus.append(swapped(plus[-1], 1))
        plus.append(from_pair)
    far = from_afar(plus[2], minus[2])
    others = shifted(sources, "xl", 1)
    pots = pltpu.VMEM((COLS, LANES), F32)
    norms = [jax.ShapeDtypeStruct((TILES, LANES), F32), jax.ShapeDtypeStruct((2, LANES), F32)]
    tile, x, state, src_norm, dst_norm = call(start_kernel, (sources, packed), [TILE, PARTS, STATE, *norms], 1, [pots])

    def own(step):
        return call(
            functools.partial(own_kernel, (-step, step)),
            (x, minus[step], plus[step], tile, state),
            [TILE, STATE],
            2,
            [pltpu.VMEM((2, COLS, LANES), F32)],
            {3: 0, 4: 1},
        )

    def partner(fresh, work, *blocks):
        first = (others,) if fresh else ()
        at = len(first) + len(blocks)
        return call(
            functools.partial(partner_kernel, fresh, work),
            (*first, *blocks, tile, x, state),
            [TILE, PARTS, STATE],
            sum(a + b for _, a, b in work),
            [pltpu.VMEM((len(work), COLS, LANES), F32)],
            {at: 0, at + 1: 1, at + 2: 2},
        )

    tile, state = own(1)
    work = ((0, 0, 1), (-1, 0, 1), (1, 0, 1), (-2, 1, 1), (2, 1, 1))
    tile, x, state = partner(True, work, packed, minus[1], plus[1], minus[2], plus[2])
    tile, x, state = partner(False, ((-3, 1, 1), (3, 1, 1)), minus[3], plus[3])
    tile, state, row_lse = call(
        functools.partial(last_kernel, -4), (x, far, tile, state), [TILE, STATE, ROW_LSE], 2, [pots], {2: 0, 3: 1}
    )
    (col_lse,) = columns(over_plane(row_lse), src_norm, tile, True)
    row_lse = rows(lax.all_to_all(col_lse, "z", 0, 0, tiled=True), tile)
    col_lse, source_pots = columns(over_plane(row_lse), src_norm, tile, False)
    col_lse = joined(lax.all_to_all(col_lse, "z", 0, 0, tiled=True))
    target_pots = (-math.log2(N_SRC) - col_lse) * (1.0 / SCALE) + dst_norm
    return (source_pots.reshape(ROWS), target_pots.reshape(COLS))


def solution(mesh):
    finer = Mesh(mesh.devices.reshape(2, 8, 4, 2, 2), (*BLK, *TGT))
    return jax.shard_map(
        steps,
        mesh=finer,
        in_specs=(P(BLK, None), P((*BLK, *TGT), None), P((*BLK, *TGT))),
        out_specs=(P(BLK), P((*BLK, *TGT))),
        check_vma=False,
    )
```

```python
import functools
import math

import jax
import jax.numpy as jnp
from jax import lax
from jax.experimental import pallas as pl
from jax.experimental.pallas import tpu as pltpu
from jax.sharding import Mesh
from jax.sharding import PartitionSpec as P


EPS = 0.05
SCALE = math.log2(math.e) / EPS
LOG2E = math.log2(math.e)
N_SRC = 16384
N_DST = 65536
ROWS = 1024
COLS = 256
RING = 8
PLANE = 32
LANES = 128
TILES = ROWS // LANES
MIB = 1024 * 1024

BLK = ("xl", "z")
TGT = ("y", "xh", "core")
PLANE_AXES = ("xl", "y", "xh", "core")

VMEM = pl.BlockSpec(memory_space=pltpu.VMEM)


def log2(x):
    return jnp.log(x) * LOG2E


def diagonal():
    shape = (LANES, LANES)
    return lax.broadcasted_iota(jnp.int32, shape, 0) == lax.broadcasted_iota(jnp.int32, shape, 1)


def as_column(eye, row):
    return jnp.sum(jnp.where(eye, row, 0.0), axis=1, keepdims=True)


def as_row(eye, column):
    return jnp.sum(jnp.where(eye, column, 0.0), axis=0, keepdims=True)


def tree(op, parts):
    parts = list(parts)
    while len(parts) > 1:
        parts = [op(*parts[k : k + 2]) if k + 1 < len(parts) else parts[k] for k in range(0, len(parts), 2)]
    return parts[0]


def three_parts(x):
    high = x.astype(jnp.bfloat16)
    rest = x - high.astype(jnp.float32)
    mid = rest.astype(jnp.bfloat16)
    low = (rest - mid.astype(jnp.float32)).astype(jnp.bfloat16)
    return high, mid, low


def online(scores, state):
    high = tree(jnp.maximum, scores)
    if state is None:
        return high, tree(jnp.add, [jnp.exp2(s - high) for s in scores])
    high = jnp.maximum(high, state[0])
    total = tree(jnp.add, [jnp.exp2(s - high) for s in scores])
    return high, state[1] * jnp.exp2(state[0] - high) + total


def over_sublanes(high, total):
    top = jnp.max(high, axis=0, keepdims=True)
    return top + log2(jnp.sum(total * jnp.exp2(high - top), axis=0, keepdims=True))


def joined(parts):
    top = jnp.max(parts, axis=0)
    return top + log2(jnp.sum(jnp.exp2(parts - top[None]), axis=0))


def put_rows(rows_ref, state_of):
    for half in range(2):
        lse = jnp.concatenate([over_sublanes(*state_of(half, t)) for t in range(TILES)], axis=0)
        for peer in range(PLANE):
            rows_ref[peer, half] = lse


def prepare_sources(x, half, x_ref):
    turned = (x * (2.0 * SCALE)).T
    high, mid, low = three_parts(turned)
    for k, part in enumerate((high, high, mid, mid, low, high)):
        x_ref[half, k * LANES : (k + 1) * LANES, :] = part


def prepare_targets(eye, block_ref, pots_ref):
    y = block_ref[0:COLS, :]
    norms = jnp.sum(y * y, axis=1, keepdims=True)
    for c in range(COLS // LANES):
        rows = slice(c * LANES, (c + 1) * LANES)
        column = as_column(eye, block_ref[COLS + c : COLS + c + 1, :])
        pots_ref[rows, :] = jnp.broadcast_to((column - norms[rows]) * SCALE, (LANES, LANES))
    high, mid, low = three_parts(y)
    return jnp.concatenate([high, mid, high, mid, high, low], axis=1), norms


def add_block(parts, pots_ref, at, half, x_ref, tile_ref, state_ref, fresh):
    step = 512
    for n in range(ROWS // step):
        lanes = slice(n * step, (n + 1) * step)
        tile_ref[at, half, :, lanes] = jnp.dot(parts, x_ref[half, :, lanes], preferred_element_type=jnp.float32)
        for t in range(n * step // LANES, (n + 1) * step // LANES):
            tile = slice(t * LANES, (t + 1) * LANES)
            state = None if fresh else (state_ref[0, half, :, tile], state_ref[1, half, :, tile])
            for c in range(0, COLS, 64):
                rows = range(c, c + 64, 8)
                state = online([tile_ref[at, half, r : r + 8, tile] + pots_ref[r : r + 8, :] for r in rows], state)
            state_ref[0, half, :, tile], state_ref[1, half, :, tile] = state


def ring_index(z, offset):
    return lax.rem(z + jnp.where(lax.rem(z, 2) == 0, offset, -offset) + RING, RING)


def start_kernel(sources_ref, block_ref, tile_ref, x_ref, state_ref, src_norm_ref, dst_norm_ref, pots_scr):
    z, mine = lax.axis_index("z"), lax.axis_index("xl")
    eye = diagonal()
    x = sources_ref[...]
    prepare_sources(x, mine, x_ref)
    squares = jnp.sum(x * x, axis=1, keepdims=True)
    for c in range(TILES):
        src_norm_ref[c : c + 1, :] = as_row(eye, squares[c * LANES : (c + 1) * LANES])
    parts, norms = prepare_targets(eye, block_ref, pots_scr)
    for c in range(COLS // LANES):
        dst_norm_ref[c : c + 1, :] = as_row(eye, norms[c * LANES : (c + 1) * LANES])
    add_block(parts, pots_scr, z, mine, x_ref, tile_ref, state_ref, True)


def own_kernel(x_ref, packed_ref, minus_ref, plus_ref, *refs):
    tile_ref, state_ref, kept_ref, pots_ref = refs[2:]
    z, mine = lax.axis_index("z"), lax.axis_index("xl")
    eye = diagonal()
    for b, (block_ref, offset) in enumerate(((packed_ref, 0), (minus_ref, -1), (plus_ref, 1))):
        parts, _ = prepare_targets(eye, block_ref, pots_ref.at[b])
        kept_ref[b] = parts
        if offset:
            add_block(parts, pots_ref.at[b], ring_index(z, offset), mine, x_ref, tile_ref, state_ref, False)


def partner_kernel(fresh, work, *refs):
    refs = list(refs)
    ready = 0
    if fresh:
        sources_ref, kept_ref, kept_pots_ref = refs.pop(0), refs.pop(0), refs.pop(0)
        ready = kept_ref.shape[0]
    blocks, (tile_ref, x_ref, state_ref), pots_scr = refs[: len(work) - ready], refs[-4:-1], refs[-1]
    z, mine = lax.axis_index("z"), lax.axis_index("xl")
    eye = diagonal()
    if fresh:
        prepare_sources(sources_ref[...], 1 - mine, x_ref)
    for b, (offset, own, partner) in enumerate(work):
        if b < ready:
            parts, pots_ref = kept_ref[b], kept_pots_ref.at[b]
        else:
            pots_ref = pots_scr.at[b]
            parts, _ = prepare_targets(eye, blocks[b - ready], pots_ref)
        at = ring_index(z, offset)
        if own:
            add_block(parts, pots_ref, at, mine, x_ref, tile_ref, state_ref, False)
        if partner:
            add_block(parts, pots_ref, at, 1 - mine, x_ref, tile_ref, state_ref, fresh and b == 0)


def last_kernel(offset, x_ref, block_ref, *refs):
    (tile_ref, state_ref, rows_ref), pots_scr = refs[-4:-1], refs[-1]
    parts, _ = prepare_targets(diagonal(), block_ref, pots_scr)
    for half in range(2):
        add_block(parts, pots_scr, ring_index(lax.axis_index("z"), offset), half, x_ref, tile_ref, state_ref, False)
    tiles = [slice(t * LANES, (t + 1) * LANES) for t in range(TILES)]
    put_rows(rows_ref, lambda half, t: (state_ref[0, half, :, tiles[t]], state_ref[1, half, :, tiles[t]]))


F32 = jnp.float32
TILE = jax.ShapeDtypeStruct((RING, 2, COLS, ROWS), F32)
PARTS = jax.ShapeDtypeStruct((2, 6 * LANES, ROWS), jnp.bfloat16)
STATE = jax.ShapeDtypeStruct((2, 2, 8, ROWS), F32)
ROW_LSE = jax.ShapeDtypeStruct((PLANE, 2, TILES, LANES), F32)


def call(kernel, args, outs, blocks, scratch=(), aliases={}):
    return pl.pallas_call(
        kernel,
        out_shape=outs,
        in_specs=[VMEM] * len(args),
        out_specs=[VMEM] * len(outs),
        scratch_shapes=list(scratch),
        input_output_aliases=aliases,
        compiler_params=pltpu.CompilerParams(vmem_limit_bytes=24 * MIB),
        cost_estimate=pl.CostEstimate(
            flops=blocks * 2 * COLS * ROWS * 768, bytes_accessed=MIB, transcendentals=blocks * COLS * ROWS
        ),
    )(*args)


def pick_kernel(plus_ref, minus_ref, far_ref):
    odd = lax.rem(lax.axis_index("z") + lax.axis_index("core"), 2) == 1
    far_ref[...] = jnp.where(odd, plus_ref[...], minus_ref[...])


def from_afar(plus, minus):
    (block,) = call(pick_kernel, (plus, minus), [jax.ShapeDtypeStruct(plus.shape, F32)], 0)
    pairs = [(2 * z + c, 2 * ((z + (2, -2)[c]) % RING) + c) for z in range(RING) for c in range(2)]
    return lax.ppermute(block, ("z", "core"), pairs)


def columns_kernel(copies, rows_ref, src_norm_ref, tile_ref, *refs):
    if copies:
        cols_ref, part_scr, turned_scr = refs
    else:
        cols_ref, source_pots_ref, part_scr, turned_scr = refs
    u = -math.log2(N_DST) - joined(rows_ref[...])
    if not copies:
        mine = lax.axis_index("xl")
        own = jnp.where(mine == 0, u[0], u[1])
        source_pots_ref[...] = own * (1.0 / SCALE) + src_norm_ref[...]
    pots = [jnp.broadcast_to(u[h, t : t + 1, :], (8, LANES)) for h in range(2) for t in range(TILES)]
    groups = 32
    turns = COLS // 8 // groups

    def load(i, g, h):
        k, first = i // turns, lax.rem(i, turns) * (8 * groups)
        rows = pl.ds(pl.multiple_of(first + 8 * g, 8), 8)
        scores = [tile_ref[k, h, rows, t * LANES : (t + 1) * LANES] + pots[h * TILES + t] for t in range(TILES)]
        return tree(jnp.maximum, scores), scores

    def turn(k, quarter):
        turned_scr[k, quarter] = part_scr[k, quarter].T

    def body(i, held):
        k, place = i // turns, lax.rem(i, turns)
        for quarter in range(4 // turns):
            turn(jnp.maximum(k - 1, 0), place * (4 // turns) + quarter)
        for g in range(groups):
            following = load(i, g, 1)
            high, scores = held
            total = tree(jnp.add, [jnp.exp2(s - high) for s in scores])
            held = following
            following = load(i, g + 1, 0) if g + 1 < groups else load(jnp.minimum(i + 1, RING * turns - 1), 0, 0)
            both, scores = jnp.maximum(high, held[0]), held[1]
            total = total * jnp.exp2(high - both) + tree(jnp.add, [jnp.exp2(s - both) for s in scores])
            half, rows = place + g // 16, slice(8 * (g % 16), 8 * (g % 16) + 8)
            part_scr[k, half, rows, :] = both
            part_scr[k, 2 + half, rows, :] = total
            held = following
        return held

    lax.fori_loop(0, RING * turns, body, load(0, 0, 0))
    for quarter in range(4):
        turn(RING - 1, quarter)
    for k in range(RING):
        for c in range(2):
            high = turned_scr[k, c]
            top = jnp.max(high, axis=0, keepdims=True)
            total = jnp.sum(turned_scr[k, 2 + c] * jnp.exp2(high - top), axis=0, keepdims=True)
            lse = top + log2(total)
            if copies:
                for peer in range(RING):
                    cols_ref[peer, 2 * k + c : 2 * k + c + 1, :] = lse
            else:
                cols_ref[k, c : c + 1, :] = lse


def columns(rows, src_norm, tile, copies):
    if copies:
        outs = [jax.ShapeDtypeStruct((RING, RING * 2, LANES), F32)]
    else:
        outs = [jax.ShapeDtypeStruct((RING, 2, LANES), F32), jax.ShapeDtypeStruct((TILES, LANES), F32)]
    scratch = [pltpu.VMEM((RING, 4, LANES, LANES), F32)] * 2
    return call(functools.partial(columns_kernel, copies), (rows, src_norm, tile), outs, 16, scratch)


def rows_kernel(cols_ref, tile_ref, rows_ref, w_scr, pots_scr, high_scr, total_scr):
    eye = diagonal()
    w_scr[...] = (-math.log2(N_SRC) - joined(cols_ref[...])).reshape(RING, 2, LANES)
    high_scr[...] = jnp.full_like(high_scr, -3.0e38)
    total_scr[...] = jnp.zeros_like(total_scr)

    def spread(k, slot):
        for c in range(2):
            column = as_column(eye, w_scr[k, c : c + 1, :])
            pots_scr[slot, c * LANES : (c + 1) * LANES, :] = jnp.broadcast_to(column, (LANES, LANES))

    def block(k, slot):
        for half in range(2):
            for t in range(TILES):
                tile = slice(t * LANES, (t + 1) * LANES)
                state = high_scr[half, :, tile], total_scr[half, :, tile]
                for c in range(0, COLS, 64):
                    rows = range(c, c + 64, 8)
                    scores = [tile_ref[k, half, r : r + 8, tile] + pots_scr[slot, r : r + 8, :] for r in rows]
                    state = online(scores, state)
                high_scr[half, :, tile], total_scr[half, :, tile] = state

    def two_blocks(i, carry):
        spread(2 * i + 1, 1)
        block(2 * i, 0)
        spread(jnp.minimum(2 * i + 2, RING - 1), 0)
        block(2 * i + 1, 1)
        return carry

    spread(0, 0)
    lax.fori_loop(0, RING // 2, two_blocks, 0)
    tiles = [slice(t * LANES, (t + 1) * LANES) for t in range(TILES)]
    put_rows(rows_ref, lambda half, t: (high_scr[half, :, tiles[t]], total_scr[half, :, tiles[t]]))


def rows(cols, tile):
    scratch = [
        pltpu.VMEM((RING, 2, LANES), F32),
        pltpu.VMEM((2, COLS, LANES), F32),
        pltpu.VMEM((2, 8, ROWS), F32),
        pltpu.VMEM((2, 8, ROWS), F32),
    ]
    return call(rows_kernel, (cols, tile), [ROW_LSE], 16, scratch)[0]


def shifted(x, axis, by):
    count = lax.axis_size(axis)
    return lax.ppermute(x, axis, [(i, (i + by) % count) for i in range(count)])


def swapped(x, first):
    pairs = [(z, (z + (1 if z % 2 == first else -1)) % RING) for z in range(RING)]
    return lax.ppermute(x, "z", pairs)


def over_plane(copies):
    return lax.all_to_all(copies, PLANE_AXES, 0, 0, tiled=True)


def steps(sources, targets, duals_init):
    packed = jnp.concatenate([targets, jnp.pad(duals_init.reshape(2, LANES), ((0, 6), (0, 0)))], axis=0)
    plus, minus = [packed], [packed]
    for _ in range(1, RING // 2):
        from_pair = swapped(minus[-1], 0)
        minus.append(swapped(plus[-1], 1))
        plus.append(from_pair)
    far = from_afar(plus[2], minus[2])
    others = shifted(sources, "xl", 1)
    pots = pltpu.VMEM((COLS, LANES), F32)
    norms = [jax.ShapeDtypeStruct((TILES, LANES), F32), jax.ShapeDtypeStruct((2, LANES), F32)]
    tile, x, state, src_norm, dst_norm = call(start_kernel, (sources, packed), [TILE, PARTS, STATE, *norms], 1, [pots])
    kept = [jax.ShapeDtypeStruct((3, COLS, 6 * LANES), jnp.bfloat16), jax.ShapeDtypeStruct((3, COLS, LANES), F32)]
    tile, state, *kept = call(
        own_kernel, (x, packed, minus[1], plus[1], tile, state), [TILE, STATE, *kept], 2, (), {4: 0, 5: 1}
    )

    def partner(fresh, work, *blocks):
        first = (others, *kept) if fresh else ()
        at = len(first) + len(blocks)
        return call(
            functools.partial(partner_kernel, fresh, work),
            (*first, *blocks, tile, x, state),
            [TILE, PARTS, STATE],
            sum(a + b for _, a, b in work),
            [pltpu.VMEM((len(work), COLS, LANES), F32)],
            {at: 0, at + 1: 1, at + 2: 2},
        )

    work = ((0, 0, 1), (-1, 0, 1), (1, 0, 1), (-2, 1, 1), (2, 1, 1))
    tile, x, state = partner(True, work, minus[2], plus[2])
    tile, x, state = partner(False, ((-3, 1, 1), (3, 1, 1)), minus[3], plus[3])
    tile, state, row_lse = call(
        functools.partial(last_kernel, -4), (x, far, tile, state), [TILE, STATE, ROW_LSE], 2, [pots], {2: 0, 3: 1}
    )
    (col_lse,) = columns(over_plane(row_lse), src_norm, tile, True)
    row_lse = rows(lax.all_to_all(col_lse, "z", 0, 0, tiled=True), tile)
    col_lse, source_pots = columns(over_plane(row_lse), src_norm, tile, False)
    col_lse = joined(lax.all_to_all(col_lse, "z", 0, 0, tiled=True))
    target_pots = (-math.log2(N_SRC) - col_lse) * (1.0 / SCALE) + dst_norm
    return (source_pots.reshape(ROWS), target_pots.reshape(COLS))


def solution(mesh):
    finer = Mesh(mesh.devices.reshape(2, 8, 4, 2, 2), (*BLK, *TGT))
    return jax.shard_map(
        steps,
        mesh=finer,
        in_specs=(P(BLK, None), P((*BLK, *TGT), None), P((*BLK, *TGT))),
        out_specs=(P(BLK), P((*BLK, *TGT))),
        check_vma=False,
    )
```
